256 devices in a mesh: groups: 2 (over z), dp: 128 (over y, x, core).
Axes of the slice: x: 8, y: 8, z: 2, core: 2. Of those that a mesh axis runs over, the one named last changes fastest.
The devices are a block of a 8x8x16 slice.
Arguments:
- batch_counts: int32 [256], P(('groups', 'dp')), parts along dimension 0, may hold values from 1 to 4, 256 in all
- attn_out: bfloat16 [1024, 7168], P(('groups', 'dp')), parts along dimension 0, may hold values from -6 to 6
- residual_in: bfloat16 [1024, 7168], P(('groups', 'dp')), parts along dimension 0, may hold values from -64 to 64
- norm_gain: float32 [7168], replicated, may hold values from 0.5 to 1.5
- w_gate_up: bfloat16 [2, 18432, 7168], P(None, 'dp'), may hold values from -0.0625 to 0.0625
- w_down: bfloat16 [18432, 7168], P(None, 'dp'), may hold values from -0.046875 to 0.046875
- next_gain: float32 [7168], replicated, may hold values from 0.5 to 1.5
Outputs:
- hidden_out: bfloat16 [1024, 7168], P(('groups', 'dp')), parts along dimension 0
- normed_out: bfloat16 [1024, 7168], P(('groups', 'dp')), parts along dimension 0
The draws below stay inside these ranges and needn't reach their ends.
There are 2 independent parts, one for each index of `groups`. The reference program is written for one: setup_inputs(seed, part) draws one part's arguments, and reference() takes and returns one part's arrays. A program takes and returns all parts, laid end to end along the dimension named above; an argument that names none is the same for every part. Nothing has to cross between parts.
Inputs may be any that keep to these rules, and one draw needn't show every extreme that they name: Rank r's occupied rows are its first batch_counts[r] slots; the counts sum to exactly 256, and some rank holds 4.
All inputs are finite; a program needn't handle non-finite values. No bound on the sum of `batch_counts` on one device may be relied on, other than what follows from the above.
Results may differ from the reference program's by a relative error of at most 0.0045.
Values may be sent and summed in bfloat16 or wider, within the bound.
No kernel may reach another device: no remote copies, remote signals or barrier semaphores. Data moves between devices by JAX's collectives and lax.ppermute only.
A program may use at most 64 MiB of HBM per device.

```python
import math
import jax
import jax.numpy as jnp
import numpy as np
from jax import lax

D = 7168
FF = 18432
SLOTS = 4
ROWS = 512
TOKENS = 256
N_DP = 128


def draw_residual_in(key, part):
    sample = jnp.clip(jax.random.normal(jax.random.fold_in(key, 37), (ROWS, D), jnp.float32), -5.0, 5.0)
    row_scale = jnp.exp(jax.random.uniform(jax.random.fold_in(key, 41), (ROWS, 1), jnp.float32, math.log(0.3), math.log(3.0)))
    col_scale = jnp.exp(jax.random.uniform(jax.random.fold_in(key, 43), (1, D), jnp.float32, math.log(0.3), math.log(3.0)))
    return (sample * row_scale * col_scale).astype(jnp.bfloat16)


def block_scale(key, extent, pieces, smallest, largest):
    def one(axis_at, parts):
        draws = jax.random.uniform(jax.random.fold_in(jax.random.fold_in(key, 6), axis_at), (parts,), jnp.float32, smallest / len(pieces), largest / len(pieces))
        return jnp.repeat(jnp.exp(draws), extent[axis_at] // parts).reshape((-1,) + (1,) * (len(extent) - axis_at - 1))

    level = one(*pieces[0])
    for cut in pieces[1:]:
        level = level * one(*cut)
    return level


def profile(count, total, bound, skew):
    loads = [(1 << 20) // math.isqrt(grade ** skew) + 1 for grade in range(2, count + 1)]
    rest, holding = total - bound - (count - 1), [1] * (count - 1)
    while rest > 0:
        candidates = [i for i in range(count - 1) if holding[i] < bound]
        pool, left = sum([loads[i] for i in candidates]), rest
        for i in candidates:
            more = min(bound - holding[i], max(1, left * loads[i] // pool), rest)
            holding[i] = holding[i] + more
            rest = rest - more
    return np.array([bound] + holding)


def ragged_sizes(stream_key, amount, total, reach, lean):
    if amount == 2:
        one = jax.random.randint(stream_key, (), max(1, total - reach), min(reach, total - 1) + 1)
        return jnp.stack([one, total - one])
    tallies = jnp.asarray(profile(amount, total, reach, lean), jnp.int32)
    twos = (amount - 1) // 2
    source_of, sink = tallies[1:1 + 2 * twos:2], tallies[2:2 + 2 * twos:2]
    margin = jnp.minimum(source_of - 1, reach - sink)
    passed = jax.random.randint(jax.random.fold_in(stream_key, 1), (twos,), 0, 1 << 20) % (margin + 1)
    tallies = tallies.at[1:1 + 2 * twos:2].set(source_of - passed).at[2:2 + 2 * twos:2].set(sink + passed)
    return tallies[jax.random.permutation(jax.random.fold_in(stream_key, 2), amount)]


def noise(stream_key, shape, scale, most, split=(), kind=jnp.bfloat16):
    gain = block_scale(stream_key, shape, split, -0.22, 0.18) if split else 1.0
    entries = jax.random.normal(stream_key, shape, jnp.float32) * scale * gain
    return jnp.minimum(jnp.maximum(entries, -most), most).astype(kind)


def setup_inputs(seed: int = 0, part: int = 0) -> dict:
    arg_keys = jax.random.split(jax.random.key(seed), 8)
    part_splits = jax.random.split(jax.random.fold_in(arg_keys[7], part), 8)
    return {
        "batch_counts": ragged_sizes(part_splits[0], N_DP, TOKENS, SLOTS, 2).astype(jnp.int32),
        "attn_out": noise(part_splits[1], (ROWS, D), 1.0, 6.0, ((0, 128),)),
        "residual_in": draw_residual_in(jax.random.fold_in(jax.random.fold_in(arg_keys[7], part), 71), part),
        "norm_gain": jnp.clip(1.0 + 0.1 * jax.random.normal(arg_keys[3], (D,), jnp.float32), 0.5, 1.5),
        "w_gate_up": noise(arg_keys[4], (2, FF, D), D ** -0.5, 0.0625, ((1, 128),)),
        "w_down": noise(arg_keys[5], (FF, D), FF ** -0.5, 0.046875, ((1, 128),)),
        "next_gain": jnp.clip(1.0 + 0.1 * jax.random.normal(arg_keys[6], (D,), jnp.float32), 0.5, 1.5),
    }


EPSILON = 1e-06

def normalize(values, weight_gain):
    mean_square = lax.optimization_barrier(jnp.mean(values * values, axis=-1, keepdims=True))
    return values * lax.rsqrt(mean_square + EPSILON) * weight_gain

def reference(batch_counts, attn_out, residual_in, norm_gain, w_gate_up, w_down, next_gain):
    slot_index = jnp.arange(ROWS, dtype=jnp.int32)
    occupied = slot_index % SLOTS < jnp.repeat(batch_counts.astype(jnp.int32), SLOTS)
    summed = residual_in.astype(jnp.float32) + attn_out.astype(jnp.float32)
    normed_in = normalize(summed, norm_gain).astype(jnp.bfloat16)
    picked = jnp.nonzero(occupied, size=TOKENS)[0].astype(jnp.int32)
    picked_rows = normed_in[picked]
    gate_part = jnp.dot(picked_rows, w_gate_up[0].T, preferred_element_type=jnp.float32)
    up_part = jnp.dot(picked_rows, w_gate_up[1].T, preferred_element_type=jnp.float32)
    activated = (jax.nn.silu(gate_part) * up_part).astype(jnp.bfloat16)
    mlp_rows = jnp.dot(activated, w_down, preferred_element_type=jnp.float32).astype(jnp.bfloat16)
    mlp_out = jnp.zeros((ROWS, mlp_rows.shape[1]), jnp.bfloat16).at[picked].set(mlp_rows)
    updated = summed + mlp_out.astype(jnp.float32)
    hidden_out = jnp.where(occupied[:, None], updated, 0.0).astype(jnp.bfloat16)
    normed_out = jnp.where(occupied[:, None], normalize(updated, next_gain), 0.0).astype(jnp.bfloat16)
    return (hidden_out, normed_out)
```

```python
import math

import jax
import jax.numpy as jnp
from jax import lax
from jax.sharding import Mesh, PartitionSpec as P

EPSILON = 1e-06
CORES = 2


def normalize(values, weight_gain):
    mean_square = jnp.mean(values * values, axis=-1, keepdims=True)
    return values * lax.rsqrt(mean_square + EPSILON) * weight_gain


def shift(extent, by):
    return [(i, (i + by) % extent) for i in range(extent)]


def ring_gather(block, axis, extent):
    found = {0: block}
    ahead = back = block
    for hop in range(1, extent // 2 + 1):
        ahead = lax.ppermute(ahead, axis, shift(extent, 1))
        found[hop] = ahead
        if hop < extent - hop:
            back = lax.ppermute(back, axis, shift(extent, -1))
            found[extent - hop] = back
    return found


def build(side):
    def on_device(batch_counts, attn_out, residual_in, norm_gain, w_gate_up, w_down, next_gain):
        slots, width = attn_out.shape
        units = w_gate_up.shape[1]
        feats = w_down.shape[1]
        x_at = lax.axis_index("x")
        core = lax.axis_index("core")
        swap = [(0, 1), (1, 0)]

        partner_gate_up = lax.ppermute(w_gate_up, "core", swap)

        occupied = lax.broadcasted_iota(jnp.int32, (slots, 1), 0) < batch_counts[0]
        summed = residual_in.astype(jnp.float32) + attn_out.astype(jnp.float32)
        normed_in = normalize(summed, norm_gain).astype(jnp.bfloat16)

        column = lax.all_to_all(
            jnp.broadcast_to(normed_in[None], (side, slots, width)), "y", split_axis=0, concat_axis=0, tiled=True
        ).reshape(side * slots, width)

        by_line = w_down.T.reshape(feats, side, side * CORES * units).transpose(1, 0, 2)
        line_down = lax.all_to_all(by_line, "y", split_axis=0, concat_axis=0, tiled=True)
        line_down = line_down.reshape(side * feats, side * CORES * units)
        partner_down = lax.ppermute(line_down, "core", swap)

        def hidden(rows):
            def part(weights):
                both = jnp.einsum("rd,gfd->grf", rows, weights, preferred_element_type=jnp.float32)
                return (jax.nn.silu(both[0]) * both[1]).astype(jnp.bfloat16)

            own, other = part(w_gate_up), part(partner_gate_up)
            return jnp.where(core == 0, jnp.concatenate([own, other], 1), jnp.concatenate([other, own], 1))

        columns = ring_gather(column, "x", side)
        acts = jnp.concatenate([hidden(columns[k]) for k in range(side)], axis=0)
        acts = acts.reshape(side, side * slots, CORES * units)
        acts = jnp.take(acts, (x_at - jnp.arange(side)) % side, axis=0)
        acts = acts.reshape(side * side * slots, CORES * units)

        blocks = ring_gather(acts, "x", side)
        down = jnp.concatenate([line_down, partner_down], 0).reshape(CORES * side * feats, side, CORES * units)
        partial = jnp.zeros((side * side * slots, CORES * side * feats), jnp.float32)
        for k in range(side):
            rows_of = lax.dynamic_index_in_dim(down, (x_at - k) % side, 1, keepdims=False)
            partial = partial + lax.dot_general(
                blocks[k], rows_of, (((1,), (1,)), ((), ())), preferred_element_type=jnp.float32
            )
        outgoing = partial.astype(jnp.bfloat16).reshape(side, side, slots, CORES * side * feats)
        outgoing = outgoing.transpose(1, 0, 2, 3)
        arrived = lax.all_to_all(outgoing, "y", split_axis=0, concat_axis=0, tiled=True)
        line_sum = jnp.sum(arrived.astype(jnp.float32), axis=0).astype(jnp.bfloat16)
        mine = lax.all_to_all(line_sum, "x", split_axis=0, concat_axis=0, tiled=True)
        mine = mine.reshape(side, slots, CORES, side, feats)
        mine = jnp.where(core == 0, mine, mine[:, :, ::-1])
        mlp_out = mine.transpose(1, 3, 0, 2, 4).reshape(slots, width)

        updated = summed + mlp_out.astype(jnp.float32)
        hidden_out = jnp.where(occupied, updated, 0.0).astype(jnp.bfloat16)
        normed_out = jnp.where(occupied, normalize(updated, next_gain), 0.0).astype(jnp.bfloat16)
        return (hidden_out, normed_out)

    return on_device


def solution(mesh):
    side = math.isqrt(mesh.shape["dp"] // CORES)
    fine = Mesh(mesh.devices.reshape(mesh.shape["groups"], side, side, CORES), ("groups", "y", "x", "core"))
    dp = ("y", "x", "core")
    rows = ("groups",) + dp
    return jax.shard_map(
        build(side),
        mesh=fine,
        in_specs=(P(rows), P(rows, None), P(rows, None), P(), P(None, dp, None), P(None, dp), P()),
        out_specs=(P(rows, None), P(rows, None)),
        check_vma=False,
    )
```

```python
import math

import jax
import jax.numpy as jnp
from jax import lax
from jax.sharding import Mesh, PartitionSpec as P

EPSILON = 1e-06
CORES = 2


def normalize(values, weight_gain):
    mean_square = jnp.mean(values * values, axis=-1, keepdims=True)
    return values * lax.rsqrt(mean_square + EPSILON) * weight_gain


def shift(extent, by):
    return [(i, (i + by) % extent) for i in range(extent)]


def ring_gather(block, axis, extent, halve=True):
    found = {0: block}
    ahead = back = block
    for hop in range(1, extent // 2):
        ahead = lax.ppermute(ahead, axis, shift(extent, 1))
        back = lax.ppermute(back, axis, shift(extent, -1))
        found[hop], found[extent - hop] = ahead, back
    if halve:
        half = block.shape[0] // 2
        ahead = lax.ppermute(ahead[:half], axis, shift(extent, 1))
        back = lax.ppermute(back[half:], axis, shift(extent, -1))
        found[extent // 2] = jnp.concatenate([ahead, back], axis=0)
    else:
        found[extent // 2] = lax.ppermute(ahead, axis, shift(extent, 1))
    return found


def build(side):
    def on_device(batch_counts, attn_out, residual_in, norm_gain, w_gate_up, w_down, next_gain):
        slots, width = attn_out.shape
        units = w_gate_up.shape[1]
        feats = w_down.shape[1]
        x_at = lax.axis_index("x")
        core = lax.axis_index("core")
        swap = [(0, 1), (1, 0)]

        partner_gate_up = lax.ppermute(w_gate_up, "core", swap)

        occupied = lax.broadcasted_iota(jnp.int32, (slots, 1), 0) < batch_counts[0]
        summed = residual_in.astype(jnp.float32) + attn_out.astype(jnp.float32)
        normed_in = normalize(summed, norm_gain).astype(jnp.bfloat16)

        column = lax.all_to_all(
            jnp.broadcast_to(normed_in[None], (side, slots, width)), "y", split_axis=0, concat_axis=0, tiled=True
        ).reshape(side * slots, width)
        column, partner_gate_up = lax.optimization_barrier((column, partner_gate_up))

        by_line = w_down.T.reshape(feats, side, side * CORES * units).transpose(1, 0, 2)
        line_down = lax.all_to_all(by_line, "y", split_axis=0, concat_axis=0, tiled=True)
        line_down = line_down.reshape(side * feats, side * CORES * units)
        partner_down = lax.ppermute(line_down, "core", swap)

        def hidden(rows):
            def part(weights):
                both = jnp.einsum("rd,gfd->grf", rows, weights, preferred_element_type=jnp.float32)
                return (jax.nn.silu(both[0]) * both[1]).astype(jnp.bfloat16)

            own, other = part(w_gate_up), part(partner_gate_up)
            return jnp.concatenate([own, other], 1)

        columns = ring_gather(column, "x", side)
        acts = jnp.stack([hidden(columns[k]) for k in range(side)], axis=0)
        by_x = (x_at - jnp.arange(side)) % side
        acts = jnp.take(acts, by_x, axis=0).reshape(side * side * slots, CORES, units)
        acts = jnp.where(core == 0, acts, acts[:, ::-1])
        acts = acts.reshape(side * side * slots, CORES * units).T

        blocks = ring_gather(acts, "x", side, halve=False)
        line = jnp.take(jnp.stack([blocks[k] for k in range(side)], axis=0), by_x, axis=0)
        line = line.reshape(side * CORES * units, side * side * slots)
        partial = [
            lax.dot_general(line, down, (((0,), (1,)), ((), ())), preferred_element_type=jnp.float32)
            for down in (line_down, partner_down)
        ]
        outgoing = jnp.concatenate([p.astype(jnp.bfloat16) for p in partial], axis=1)
        outgoing = outgoing.reshape(side * side, slots, CORES * side * feats)
        arrived = lax.all_to_all(outgoing, ("x", "y"), split_axis=0, concat_axis=0, tiled=True)
        arrived = arrived.reshape(side, side, slots, CORES * side * feats)
        mine = jnp.sum(arrived.astype(jnp.float32), axis=1).astype(jnp.bfloat16)
        mine = mine.reshape(side, slots, CORES, side, feats)
        mine = jnp.where(core == 0, mine, mine[:, :, ::-1])
        mlp_out = mine.transpose(1, 3, 0, 2, 4).reshape(slots, width)

        updated = summed + mlp_out.astype(jnp.float32)
        hidden_out = jnp.where(occupied, updated, 0.0).astype(jnp.bfloat16)
        normed_out = jnp.where(occupied, normalize(updated, next_gain), 0.0).astype(jnp.bfloat16)
        return (hidden_out, normed_out)

    return on_device


def solution(mesh):
    side = math.isqrt(mesh.shape["dp"] // CORES)
    fine = Mesh(mesh.devices.reshape(mesh.shape["groups"], side, side, CORES), ("groups", "y", "x", "core"))
    dp = ("y", "x", "core")
    rows = ("groups",) + dp
    return jax.shard_map(
        build(side),
        mesh=fine,
        in_specs=(P(rows), P(rows, None), P(rows, None), P(), P(None, dp, None), P(None, dp), P()),
        out_specs=(P(rows, None), P(rows, None)),
        check_vma=False,
    )
```

```python
import math

import jax
import jax.numpy as jnp
from jax import lax
from jax.sharding import Mesh, PartitionSpec as P

EPSILON = 1e-06
CORES = 2
BATCHES = ((0, 1, 7), (2, 6), (3, 5), (4,))


def normalize(values, weight_gain):
    mean_square = jnp.mean(values * values, axis=-1, keepdims=True)
    return values * lax.rsqrt(mean_square + EPSILON) * weight_gain


def shift(extent, by):
    return [(i, (i + by) % extent) for i in range(extent)]


def ring_gather(block, axis, extent, halve=True):
    found = {0: block}
    ahead = back = block
    for hop in range(1, extent // 2):
        ahead = lax.ppermute(ahead, axis, shift(extent, 1))
        back = lax.ppermute(back, axis, shift(extent, -1))
        found[hop], found[extent - hop] = ahead, back
    if halve:
        half = block.shape[0] // 2
        ahead = lax.ppermute(ahead[:half], axis, shift(extent, 1))
        back = lax.ppermute(back[half:], axis, shift(extent, -1))
        found[extent // 2] = jnp.concatenate([ahead, back], axis=0)
    else:
        found[extent // 2] = lax.ppermute(ahead, axis, shift(extent, 1))
    return found


def build(side):
    def on_device(batch_counts, attn_out, residual_in, norm_gain, w_gate_up, w_down, next_gain):
        slots, width = attn_out.shape
        units = w_gate_up.shape[1]
        feats = w_down.shape[1]
        x_at = lax.axis_index("x")
        core = lax.axis_index("core")
        swap = [(0, 1), (1, 0)]

        partner_gate_up = lax.ppermute(w_gate_up, "core", swap)

        occupied = lax.broadcasted_iota(jnp.int32, (slots, 1), 0) < batch_counts[0]
        summed = residual_in.astype(jnp.float32) + attn_out.astype(jnp.float32)
        normed_in = normalize(summed, norm_gain).astype(jnp.bfloat16)

        column = lax.all_to_all(
            jnp.broadcast_to(normed_in[None], (side, slots, width)), "y", split_axis=0, concat_axis=0, tiled=True
        ).reshape(side * slots, width)
        column, partner_gate_up = lax.optimization_barrier((column, partner_gate_up))

        by_line = w_down.T.reshape(feats, side, side * CORES * units).transpose(1, 0, 2)
        line_down = lax.all_to_all(by_line, "y", split_axis=0, concat_axis=0, tiled=True)
        line_down = line_down.reshape(side * feats, side * CORES * units)
        partner_down = lax.ppermute(line_down, "core", swap)

        def hidden(rows):
            def part(weights):
                both = jnp.einsum("rd,gfd->grf", rows, weights, preferred_element_type=jnp.float32)
                return (jax.nn.silu(both[0]) * both[1]).astype(jnp.bfloat16)

            return part(w_gate_up), part(partner_gate_up)

        def place(blocks, shape):
            whole = jnp.zeros((side,) + shape, jnp.bfloat16)
            for k in range(side):
                whole = lax.dynamic_update_index_in_dim(whole, blocks[k], (x_at - k) % side, 0)
            return whole

        columns = ring_gather(column, "x", side)
        rows = side * slots
        own, other = {}, {}
        for batch in BATCHES:
            here, there = hidden(jnp.concatenate([columns[k] for k in batch], axis=0))
            for i, k in enumerate(batch):
                own[k] = here[i * rows : (i + 1) * rows]
                other[k] = there[i * rows : (i + 1) * rows]
        halves = [place(part, (rows, units)).reshape(side * rows, units).T for part in (own, other)]
        acts = jnp.zeros((CORES, units, side * rows), jnp.bfloat16)
        acts = lax.dynamic_update_index_in_dim(acts, halves[0], core, 0)
        acts = lax.dynamic_update_index_in_dim(acts, halves[1], 1 - core, 0)
        acts = acts.reshape(CORES * units, side * rows)

        line = place(ring_gather(acts, "x", side, halve=False), acts.shape)
        line = line.reshape(side * CORES * units, side * rows)
        partial = [
            lax.dot_general(line, down, (((0,), (1,)), ((), ())), preferred_element_type=jnp.float32)
            for down in (line_down, partner_down)
        ]
        outgoing = jnp.concatenate([p.astype(jnp.bfloat16) for p in partial], axis=1)
        outgoing = outgoing.reshape(side * side, slots, CORES * side * feats)
        arrived = lax.all_to_all(outgoing, ("x", "y"), split_axis=0, concat_axis=0, tiled=True)
        arrived = arrived.reshape(side, side, slots, CORES * side * feats)
        mine = jnp.sum(arrived.astype(jnp.float32), axis=1).astype(jnp.bfloat16)
        mine = mine.reshape(side, slots, CORES, side, feats)
        mine = jnp.where(core == 0, mine, mine[:, :, ::-1])
        mlp_out = mine.transpose(1, 3, 0, 2, 4).reshape(slots, width)

        updated = summed + mlp_out.astype(jnp.float32)
        hidden_out = jnp.where(occupied, updated, 0.0).astype(jnp.bfloat16)
        normed_out = jnp.where(occupied, normalize(updated, next_gain), 0.0).astype(jnp.bfloat16)
        return (hidden_out, normed_out)

    return on_device


def solution(mesh):
    side = math.isqrt(mesh.shape["dp"] // CORES)
    fine = Mesh(mesh.devices.reshape(mesh.shape["groups"], side, side, CORES), ("groups", "y", "x", "core"))
    dp = ("y", "x", "core")
    rows = ("groups",) + dp
    return jax.shard_map(
        build(side),
        mesh=fine,
        in_specs=(P(rows), P(rows, None), P(rows, None), P(), P(None, dp, None), P(None, dp), P()),
        out_specs=(P(rows, None), P(rows, None)),
        check_vma=False,
    )
```

```python
import functools
import math

import jax
import jax.numpy as jnp
from jax import lax
from jax.experimental import pallas as pl
from jax.experimental.pallas import tpu as pltpu
from jax.sharding import Mesh, PartitionSpec as P

EPSILON = 1e-06
CORES = 2
BATCHES = ((0, 1, 7), (2, 6), (3, 5), (4,))


def normalize(values, weight_gain):
    mean_square = jnp.mean(values * values, axis=-1, keepdims=True)
    return values * lax.rsqrt(mean_square + EPSILON) * weight_gain


CHUNK = 1024


def gate_up_body(count, *refs):
    blocks, (own, other, own_out, other_out, sums) = refs[:count], refs[count:]
    step = pl.program_id(0)
    units = own.shape[1]

    @pl.when(step == 0)
    def _():
        sums[...] = jnp.zeros_like(sums)

    rows = jnp.concatenate([block[...] for block in blocks], axis=0)
    for i, weights in enumerate((own, other)):
        both = weights[...].reshape(2 * units, weights.shape[2])
        sums[i] += lax.dot_general(rows, both, (((1,), (1,)), ((), ())), preferred_element_type=jnp.float32)

    @pl.when(step == pl.num_programs(0) - 1)
    def _():
        for i, out in enumerate((own_out, other_out)):
            gate, up = sums[i, :, :units], sums[i, :, units:]
            out[...] = (jax.nn.silu(gate) * up).astype(jnp.bfloat16)


def gate_up(blocks, own, other):
    units, width = own.shape[1:]
    rows = sum(block.shape[0] for block in blocks)
    weights = pl.BlockSpec((2, units, CHUNK), lambda k: (0, 0, k))
    out = pl.BlockSpec((rows, units), lambda k: (0, 0))
    shape = jax.ShapeDtypeStruct((rows, units), jnp.bfloat16)
    return pl.pallas_call(
        functools.partial(gate_up_body, len(blocks)),
        grid=(width // CHUNK,),
        in_specs=[pl.BlockSpec((block.shape[0], CHUNK), lambda k: (0, k)) for block in blocks] + [weights, weights],
        out_specs=(out, out),
        out_shape=(shape, shape),
        scratch_shapes=[pltpu.VMEM((2, rows, 2 * units), jnp.float32)],
        compiler_params=pltpu.CompilerParams(vmem_limit_bytes=16 * 1024 * 1024),
        cost_estimate=pl.CostEstimate(
            flops=8 * rows * units * width, bytes_accessed=8 * units * width + 2 * rows * width, transcendentals=0
        ),
        name="gate_up",
    )(*blocks, own, other)


def shift(extent, by):
    return [(i, (i + by) % extent) for i in range(extent)]


def ring_gather(block, axis, extent, halve=True):
    found = {0: [block]}
    ahead = back = block
    for hop in range(1, extent // 2):
        ahead = lax.ppermute(ahead, axis, shift(extent, 1))
        back = lax.ppermute(back, axis, shift(extent, -1))
        found[hop], found[extent - hop] = [ahead], [back]
    hop = extent // 2
    half = block.shape[0] // 2
    ahead = lax.ppermute(ahead[:half] if halve else ahead, axis, shift(extent, 1))
    found[hop] = [ahead]
    if halve:
        found[hop].append(lax.ppermute(back[half:], axis, shift(extent, -1)))
    return found


def build(side):
    def on_device(batch_counts, attn_out, residual_in, norm_gain, w_gate_up, w_down, next_gain):
        slots, width = attn_out.shape
        units = w_gate_up.shape[1]
        feats = w_down.shape[1]
        x_at = lax.axis_index("x")
        core = lax.axis_index("core")
        swap = [(0, 1), (1, 0)]

        partner_gate_up = lax.ppermute(w_gate_up, "core", swap)

        occupied = lax.broadcasted_iota(jnp.int32, (slots, 1), 0) < batch_counts[0]
        summed = residual_in.astype(jnp.float32) + attn_out.astype(jnp.float32)
        normed_in = normalize(summed, norm_gain).astype(jnp.bfloat16)

        column = lax.all_to_all(
            jnp.broadcast_to(normed_in[None], (side, slots, width)), "y", split_axis=0, concat_axis=0, tiled=True
        ).reshape(side * slots, width)
        column, partner_gate_up = lax.optimization_barrier((column, partner_gate_up))

        by_line = w_down.T.reshape(feats, side, side * CORES * units).transpose(1, 0, 2)
        line_down = lax.all_to_all(by_line, "y", split_axis=0, concat_axis=0, tiled=True)
        line_down = line_down.reshape(side * feats, side * CORES * units)
        partner_down = lax.ppermute(line_down, "core", swap)

        def place(blocks, shape):
            whole = jnp.zeros((side,) + shape, jnp.bfloat16)
            for k in range(side):
                whole = lax.dynamic_update_index_in_dim(whole, blocks[k], (x_at - k) % side, 0)
            return whole

        columns = ring_gather(column, "x", side)
        rows = side * slots
        own, other = {}, {}
        for batch in BATCHES:
            here, there = gate_up([piece for k in batch for piece in columns[k]], w_gate_up, partner_gate_up)
            for i, k in enumerate(batch):
                own[k] = here[i * rows : (i + 1) * rows]
                other[k] = there[i * rows : (i + 1) * rows]
        halves = [place(part, (rows, units)).reshape(side * rows, units).T for part in (own, other)]
        acts = jnp.zeros((CORES, units, side * rows), jnp.bfloat16)
        acts = lax.dynamic_update_index_in_dim(acts, halves[0], core, 0)
        acts = lax.dynamic_update_index_in_dim(acts, halves[1], 1 - core, 0)
        acts = acts.reshape(CORES * units, side * rows)

        blocks = ring_gather(acts, "x", side, halve=False)
        line = place({k: pieces[0] for k, pieces in blocks.items()}, acts.shape)
        line = line.reshape(side * CORES * units, side * rows)
        partial = [
            lax.dot_general(line, down, (((0,), (1,)), ((), ())), preferred_element_type=jnp.float32)
            for down in (line_down, partner_down)
        ]
        outgoing = jnp.concatenate([p.astype(jnp.bfloat16) for p in partial], axis=1)
        outgoing = outgoing.reshape(side * side, slots, CORES * side * feats)
        arrived = lax.all_to_all(outgoing, ("x", "y"), split_axis=0, concat_axis=0, tiled=True)
        arrived = arrived.reshape(side, side, slots, CORES * side * feats)
        mine = jnp.sum(arrived.astype(jnp.float32), axis=1).astype(jnp.bfloat16)
        mine = mine.reshape(side, slots, CORES, side, feats)
        mine = jnp.where(core == 0, mine, mine[:, :, ::-1])
        mlp_out = mine.transpose(1, 3, 0, 2, 4).reshape(slots, width)

        updated = summed + mlp_out.astype(jnp.float32)
        hidden_out = jnp.where(occupied, updated, 0.0).astype(jnp.bfloat16)
        normed_out = jnp.where(occupied, normalize(updated, next_gain), 0.0).astype(jnp.bfloat16)
        return (hidden_out, normed_out)

    return on_device


def solution(mesh):
    side = math.isqrt(mesh.shape["dp"] // CORES)
    fine = Mesh(mesh.devices.reshape(mesh.shape["groups"], side, side, CORES), ("groups", "y", "x", "core"))
    dp = ("y", "x", "core")
    rows = ("groups",) + dp
    body = build(side)

    return jax.shard_map(
        body,
        mesh=fine,
        in_specs=(P(rows), P(rows, None), P(rows, None), P(), P(None, dp, None), P(None, dp), P()),
        out_specs=(P(rows, None), P(rows, None)),
        check_vma=False,
    )
```

```python
import functools
import math

import jax
import jax.numpy as jnp
from jax import lax
from jax.experimental import pallas as pl
from jax.experimental.pallas import tpu as pltpu
from jax.sharding import Mesh, PartitionSpec as P

EPSILON = 1e-06
CORES = 2
BATCHES = ((0, 1, 7), (2, 6), (3, 5), (4,))


def normalize(values, weight_gain):
    mean_square = jnp.mean(values * values, axis=-1, keepdims=True)
    return values * lax.rsqrt(mean_square + EPSILON) * weight_gain


def gate_up_body(count, *refs):
    blocks, (own, other, own_out, other_out) = refs[:count], refs[count:]
    units = own.shape[1]
    rows = jnp.concatenate([block[...] for block in blocks], axis=0)
    for weights, out in ((own, own_out), (other, other_out)):
        both = weights[...].reshape(2 * units, weights.shape[2])
        both = lax.dot_general(both, rows, (((1,), (1,)), ((), ())), preferred_element_type=jnp.float32)
        gate, up = both[:units], both[units:]
        out[...] = (jax.nn.silu(gate) * up).astype(jnp.bfloat16).T


def hold_body(arrived, out, done):
    copy = pltpu.make_async_copy(arrived, out, done)
    copy.start()
    copy.wait()


def hold(arrived):
    anywhere = pl.BlockSpec(memory_space=pl.ANY)
    return pl.pallas_call(
        hold_body,
        in_specs=[anywhere],
        out_specs=anywhere,
        out_shape=jax.ShapeDtypeStruct(arrived.shape, arrived.dtype),
        scratch_shapes=[pltpu.SemaphoreType.DMA],
        name="hold",
    )(arrived)


def gate_up(blocks, own, other):
    units, width = own.shape[1:]
    rows = sum(block.shape[0] for block in blocks)
    whole = pl.BlockSpec(memory_space=pltpu.VMEM)
    shape = jax.ShapeDtypeStruct((rows, units), jnp.bfloat16)
    return pl.pallas_call(
        functools.partial(gate_up_body, len(blocks)),
        in_specs=[whole] * (len(blocks) + 2),
        out_specs=(whole, whole),
        out_shape=(shape, shape),
        compiler_params=pltpu.CompilerParams(vmem_limit_bytes=24 * 1024 * 1024),
        cost_estimate=pl.CostEstimate(
            flops=8 * rows * units * width, bytes_accessed=8 * units * width + 2 * rows * width, transcendentals=0
        ),
        name="gate_up",
    )(*blocks, own, other)


def shift(extent, by):
    return [(i, (i + by) % extent) for i in range(extent)]


def ring_gather(block, axis, extent, halve=True):
    found = {0: [block]}
    ahead = back = block
    for hop in range(1, extent // 2):
        ahead = lax.ppermute(ahead, axis, shift(extent, 1))
        back = lax.ppermute(back, axis, shift(extent, -1))
        found[hop], found[extent - hop] = [ahead], [back]
    hop = extent // 2
    half = block.shape[0] // 2
    ahead = lax.ppermute(ahead[:half] if halve else ahead, axis, shift(extent, 1))
    found[hop] = [ahead]
    if halve:
        found[hop].append(lax.ppermute(back[half:], axis, shift(extent, -1)))
    return found


def build(side):
    def on_device(batch_counts, attn_out, residual_in, norm_gain, w_gate_up, w_down, next_gain):
        slots, width = attn_out.shape
        units = w_gate_up.shape[1]
        feats = w_down.shape[1]
        x_at = lax.axis_index("x")
        core = lax.axis_index("core")
        swap = [(0, 1), (1, 0)]

        partner_gate_up = lax.ppermute(w_gate_up, "core", swap)

        occupied = lax.broadcasted_iota(jnp.int32, (slots, 1), 0) < batch_counts[0]
        summed = residual_in.astype(jnp.float32) + attn_out.astype(jnp.float32)
        normed_in = normalize(summed, norm_gain).astype(jnp.bfloat16)

        column = lax.all_to_all(
            jnp.broadcast_to(normed_in[None], (side, slots, width)), "y", split_axis=0, concat_axis=0, tiled=True
        ).reshape(side * slots, width)
        column, partner_gate_up = lax.optimization_barrier((column, partner_gate_up))
        partner_gate_up = hold(partner_gate_up)

        by_line = w_down.T.reshape(feats, side, side * CORES * units).transpose(1, 0, 2)
        line_down = lax.all_to_all(by_line, "y", split_axis=0, concat_axis=0, tiled=True)
        line_down = line_down.reshape(side * feats, side * CORES * units)
        partner_down = lax.ppermute(line_down, "core", swap)

        def place(blocks, shape):
            whole = jnp.zeros((side,) + shape, jnp.bfloat16)
            for k in range(side):
                whole = lax.dynamic_update_index_in_dim(whole, blocks[k], (x_at - k) % side, 0)
            return whole

        columns = ring_gather(column, "x", side)
        rows = side * slots
        own, other = {}, {}
        for batch in BATCHES:
            here, there = gate_up([piece for k in batch for piece in columns[k]], w_gate_up, partner_gate_up)
            for i, k in enumerate(batch):
                own[k] = here[i * rows : (i + 1) * rows]
                other[k] = there[i * rows : (i + 1) * rows]
        halves = [place(part, (rows, units)).reshape(side * rows, units).T for part in (own, other)]
        acts = jnp.zeros((CORES, units, side * rows), jnp.bfloat16)
        acts = lax.dynamic_update_index_in_dim(acts, halves[0], core, 0)
        acts = lax.dynamic_update_index_in_dim(acts, halves[1], 1 - core, 0)
        acts = acts.reshape(CORES * units, side * rows)

        blocks = ring_gather(acts, "x", side, halve=False)
        line = place({k: pieces[0] for k, pieces in blocks.items()}, acts.shape)
        line = line.reshape(side * CORES * units, side * rows)
        partial = [
            lax.dot_general(line, down, (((0,), (1,)), ((), ())), preferred_element_type=jnp.float32)
            for down in (line_down, partner_down)
        ]
        outgoing = jnp.concatenate([p.astype(jnp.bfloat16) for p in partial], axis=1)
        outgoing = outgoing.reshape(side * side, slots, CORES * side * feats)
        arrived = lax.all_to_all(outgoing, ("x", "y"), split_axis=0, concat_axis=0, tiled=True)
        arrived = arrived.reshape(side, side, slots, CORES * side * feats)
        mine = jnp.sum(arrived.astype(jnp.float32), axis=1).astype(jnp.bfloat16)
        mine = mine.reshape(side, slots, CORES, side, feats)
        mine = jnp.where(core == 0, mine, mine[:, :, ::-1])
        mlp_out = mine.transpose(1, 3, 0, 2, 4).reshape(slots, width)

        updated = summed + mlp_out.astype(jnp.float32)
        hidden_out = jnp.where(occupied, updated, 0.0).astype(jnp.bfloat16)
        normed_out = jnp.where(occupied, normalize(updated, next_gain), 0.0).astype(jnp.bfloat16)
        return (hidden_out, normed_out)

    return on_device


def solution(mesh):
    side = math.isqrt(mesh.shape["dp"] // CORES)
    fine = Mesh(mesh.devices.reshape(mesh.shape["groups"], side, side, CORES), ("groups", "y", "x", "core"))
    dp = ("y", "x", "core")
    rows = ("groups",) + dp
    body = build(side)

    return jax.shard_map(
        body,
        mesh=fine,
        in_specs=(P(rows), P(rows, None), P(rows, None), P(), P(None, dp, None), P(None, dp), P()),
        out_specs=(P(rows, None), P(rows, None)),
        check_vma=False,
    )
```

```python
import functools
import math

import jax
import jax.numpy as jnp
from jax import lax
from jax.experimental import pallas as pl
from jax.experimental.pallas import tpu as pltpu
from jax.sharding import Mesh, PartitionSpec as P

EPSILON = 1e-06
CORES = 2
BATCHES = ((0, 1, 7), (2, 6), (3, 5), (4,))


def normalize(values, weight_gain):
    mean_square = jnp.mean(values * values, axis=-1, keepdims=True)
    return values * lax.rsqrt(mean_square + EPSILON) * weight_gain


def gate_up_body(count, *refs):
    blocks, (own, other, own_out, other_out) = refs[:count], refs[count:]
    units = own.shape[1]
    rows = jnp.concatenate([block[...] for block in blocks], axis=0)
    for weights, out in ((own, own_out), (other, other_out)):
        both = weights[...].reshape(2 * units, weights.shape[2])
        both = lax.dot_general(both, rows, (((1,), (1,)), ((), ())), preferred_element_type=jnp.float32)
        gate, up = both[:units], both[units:]
        out[...] = (jax.nn.silu(gate) * up).astype(jnp.bfloat16).T


def hold_body(arrived, out):
    out[...] = arrived[...]


def hold(arrived):
    block = pl.BlockSpec((1, arrived.shape[1] // 2, arrived.shape[2]), lambda i: (i // 2, i % 2, 0))
    return pl.pallas_call(
        hold_body,
        grid=(2 * arrived.shape[0],),
        in_specs=[block],
        out_specs=block,
        out_shape=jax.ShapeDtypeStruct(arrived.shape, arrived.dtype),
        name="hold",
    )(arrived)


def gate_up(blocks, own, other):
    units, width = own.shape[1:]
    rows = sum(block.shape[0] for block in blocks)
    whole = pl.BlockSpec(memory_space=pltpu.VMEM)
    shape = jax.ShapeDtypeStruct((rows, units), jnp.bfloat16)
    return pl.pallas_call(
        functools.partial(gate_up_body, len(blocks)),
        in_specs=[whole] * (len(blocks) + 2),
        out_specs=(whole, whole),
        out_shape=(shape, shape),
        compiler_params=pltpu.CompilerParams(vmem_limit_bytes=24 * 1024 * 1024),
        cost_estimate=pl.CostEstimate(
            flops=8 * rows * units * width, bytes_accessed=8 * units * width + 2 * rows * width, transcendentals=0
        ),
        name="gate_up",
    )(*blocks, own, other)


def shift(extent, by):
    return [(i, (i + by) % extent) for i in range(extent)]


def ring_gather(block, axis, extent, halve=True):
    found = {0: [block]}
    ahead = back = block
    for hop in range(1, extent // 2):
        ahead = lax.ppermute(ahead, axis, shift(extent, 1))
        back = lax.ppermute(back, axis, shift(extent, -1))
        found[hop], found[extent - hop] = [ahead], [back]
    hop = extent // 2
    half = block.shape[0] // 2
    ahead = lax.ppermute(ahead[:half] if halve else ahead, axis, shift(extent, 1))
    found[hop] = [ahead]
    if halve:
        found[hop].append(lax.ppermute(back[half:], axis, shift(extent, -1)))
    return found


def build(side):
    def on_device(batch_counts, attn_out, residual_in, norm_gain, w_gate_up, w_down, next_gain):
        slots, width = attn_out.shape
        units = w_gate_up.shape[1]
        feats = w_down.shape[1]
        x_at = lax.axis_index("x")
        core = lax.axis_index("core")
        swap = [(0, 1), (1, 0)]

        partner_gate_up = lax.ppermute(w_gate_up, "core", swap)

        occupied = lax.broadcasted_iota(jnp.int32, (slots, 1), 0) < batch_counts[0]
        summed = residual_in.astype(jnp.float32) + attn_out.astype(jnp.float32)
        normed_in = normalize(summed, norm_gain).astype(jnp.bfloat16)

        column = lax.all_to_all(
            jnp.broadcast_to(normed_in[None], (side, slots, width)), "y", split_axis=0, concat_axis=0, tiled=True
        ).reshape(side * slots, width)
        column, partner_gate_up = lax.optimization_barrier((column, partner_gate_up))
        partner_gate_up = hold(partner_gate_up)

        by_line = w_down.T.reshape(feats, side, side * CORES * units).transpose(1, 0, 2)
        line_down = lax.all_to_all(by_line, "y", split_axis=0, concat_axis=0, tiled=True)
        line_down = line_down.reshape(side * feats, side * CORES * units)
        partner_down = lax.ppermute(line_down, "core", swap)

        def place(blocks, shape):
            whole = jnp.zeros((side,) + shape, jnp.bfloat16)
            for k in range(side):
                whole = lax.dynamic_update_index_in_dim(whole, blocks[k], (x_at - k) % side, 0)
            return whole

        columns = ring_gather(column, "x", side)
        rows = side * slots
        own, other = {}, {}
        for batch in BATCHES:
            here, there = gate_up([piece for k in batch for piece in columns[k]], w_gate_up, partner_gate_up)
            for i, k in enumerate(batch):
                own[k] = here[i * rows : (i + 1) * rows]
                other[k] = there[i * rows : (i + 1) * rows]
        halves = [place(part, (rows, units)).reshape(side * rows, units).T for part in (own, other)]
        acts = jnp.zeros((CORES, units, side * rows), jnp.bfloat16)
        acts = lax.dynamic_update_index_in_dim(acts, halves[0], core, 0)
        acts = lax.dynamic_update_index_in_dim(acts, halves[1], 1 - core, 0)
        acts = acts.reshape(CORES * units, side * rows)

        blocks = ring_gather(acts, "x", side, halve=False)
        line = place({k: pieces[0] for k, pieces in blocks.items()}, acts.shape)
        line = line.reshape(side * CORES * units, side * rows)
        partial = [
            lax.dot_general(line, down, (((0,), (1,)), ((), ())), preferred_element_type=jnp.float32)
            for down in (line_down, partner_down)
        ]
        outgoing = jnp.concatenate([p.astype(jnp.bfloat16) for p in partial], axis=1)
        outgoing = outgoing.reshape(side * side, slots, CORES * side * feats)
        arrived = lax.all_to_all(outgoing, ("x", "y"), split_axis=0, concat_axis=0, tiled=True)
        arrived = arrived.reshape(side, side, slots, CORES * side * feats)
        mine = jnp.sum(arrived.astype(jnp.float32), axis=1).astype(jnp.bfloat16)
        mine = mine.reshape(side, slots, CORES, side, feats)
        mine = jnp.where(core == 0, mine, mine[:, :, ::-1])
        mlp_out = mine.transpose(1, 3, 0, 2, 4).reshape(slots, width)

        updated = summed + mlp_out.astype(jnp.float32)
        hidden_out = jnp.where(occupied, updated, 0.0).astype(jnp.bfloat16)
        normed_out = jnp.where(occupied, normalize(updated, next_gain), 0.0).astype(jnp.bfloat16)
        return (hidden_out, normed_out)

    return on_device


def solution(mesh):
    side = math.isqrt(mesh.shape["dp"] // CORES)
    fine = Mesh(mesh.devices.reshape(mesh.shape["groups"], side, side, CORES), ("groups", "y", "x", "core"))
    dp = ("y", "x", "core")
    rows = ("groups",) + dp
    body = build(side)

    return jax.shard_map(
        body,
        mesh=fine,
        in_specs=(P(rows), P(rows, None), P(rows, None), P(), P(None, dp, None), P(None, dp), P()),
        out_specs=(P(rows, None), P(rows, None)),
        check_vma=False,
    )
```

```python
import functools
import math

import jax
import jax.numpy as jnp
from jax import lax
from jax.experimental import pallas as pl
from jax.experimental.pallas import tpu as pltpu
from jax.sharding import Mesh, PartitionSpec as P

EPSILON = 1e-06
CORES = 2
BATCHES = ((0, 1, 7), (2, 6), (3, 5), (4,))


def normalize(values, weight_gain):
    mean_square = jnp.mean(values * values, axis=-1, keepdims=True)
    return values * lax.rsqrt(mean_square + EPSILON) * weight_gain


def gate_up_body(count, *refs):
    blocks, (own, other, own_out, other_out) = refs[:count], refs[count:]
    units = own.shape[1]
    rows = jnp.concatenate([block[...] for block in blocks], axis=0)
    for weights, out in ((own, own_out), (other, other_out)):
        both = weights[...].reshape(2 * units, weights.shape[2])
        both = lax.dot_general(both, rows, (((1,), (1,)), ((), ())), preferred_element_type=jnp.float32)
        gate, up = both[:units], both[units:]
        out[...] = (jax.nn.silu(gate) * up).astype(jnp.bfloat16).T


def hold_body(arrived, out):
    out[...] = arrived[...]


def hold_body_line(arrived, out):
    out[0] = arrived[...]


def hold(arrived):
    block = pl.BlockSpec((1, arrived.shape[1] // 2, arrived.shape[2]), lambda i: (i // 2, i % 2, 0))
    return pl.pallas_call(
        hold_body,
        grid=(2 * arrived.shape[0],),
        in_specs=[block],
        out_specs=block,
        out_shape=jax.ShapeDtypeStruct(arrived.shape, arrived.dtype),
        name="hold",
    )(arrived)


def split_lines(weights, lines):
    feats, units = weights.shape
    units //= lines
    return pl.pallas_call(
        hold_body_line,
        grid=(lines,),
        in_specs=[pl.BlockSpec((feats, units), lambda i: (0, i))],
        out_specs=pl.BlockSpec((1, feats, units), lambda i: (i, 0, 0)),
        out_shape=jax.ShapeDtypeStruct((lines, feats, units), weights.dtype),
        name="split_lines",
    )(weights)


def gate_up(blocks, own, other):
    units, width = own.shape[1:]
    rows = sum(block.shape[0] for block in blocks)
    whole = pl.BlockSpec(memory_space=pltpu.VMEM)
    shape = jax.ShapeDtypeStruct((rows, units), jnp.bfloat16)
    return pl.pallas_call(
        functools.partial(gate_up_body, len(blocks)),
        in_specs=[whole] * (len(blocks) + 2),
        out_specs=(whole, whole),
        out_shape=(shape, shape),
        compiler_params=pltpu.CompilerParams(vmem_limit_bytes=24 * 1024 * 1024),
        cost_estimate=pl.CostEstimate(
            flops=8 * rows * units * width, bytes_accessed=8 * units * width + 2 * rows * width, transcendentals=0
        ),
        name="gate_up",
    )(*blocks, own, other)


def shift(extent, by):
    return [(i, (i + by) % extent) for i in range(extent)]


def ring_gather(block, axis, extent, halve=True):
    found = {0: [block]}
    ahead = back = block
    for hop in range(1, extent // 2):
        ahead = lax.ppermute(ahead, axis, shift(extent, 1))
        back = lax.ppermute(back, axis, shift(extent, -1))
        found[hop], found[extent - hop] = [ahead], [back]
    hop = extent // 2
    half = block.shape[0] // 2
    ahead = lax.ppermute(ahead[:half] if halve else ahead, axis, shift(extent, 1))
    found[hop] = [ahead]
    if halve:
        found[hop].append(lax.ppermute(back[half:], axis, shift(extent, -1)))
    return found


def build(side):
    def on_device(batch_counts, attn_out, residual_in, norm_gain, w_gate_up, w_down, next_gain):
        slots, width = attn_out.shape
        units = w_gate_up.shape[1]
        feats = w_down.shape[1]
        x_at = lax.axis_index("x")
        core = lax.axis_index("core")
        swap = [(0, 1), (1, 0)]

        partner_gate_up = lax.ppermute(w_gate_up, "core", swap)

        occupied = lax.broadcasted_iota(jnp.int32, (slots, 1), 0) < batch_counts[0]
        summed = residual_in.astype(jnp.float32) + attn_out.astype(jnp.float32)
        normed_in = normalize(summed, norm_gain).astype(jnp.bfloat16)

        sent = jnp.broadcast_to(normed_in[None], (side, slots, width))
        column = lax.all_to_all(sent, "y", split_axis=0, concat_axis=0, tiled=True)
        partner_gate_up = hold(partner_gate_up)
        by_line = split_lines(w_down.T, side)
        column = column.reshape(side * slots, width)

        line_down = lax.all_to_all(by_line, "y", split_axis=0, concat_axis=0, tiled=True)
        line_down = line_down.reshape(side * feats, side * CORES * units)
        partner_down = lax.ppermute(line_down, "core", swap)

        def place(blocks, shape):
            whole = jnp.zeros((side,) + shape, jnp.bfloat16)
            for k in range(side):
                whole = lax.dynamic_update_index_in_dim(whole, blocks[k], (x_at - k) % side, 0)
            return whole

        columns = ring_gather(column, "x", side)
        rows = side * slots
        own, other = {}, {}
        for batch in BATCHES:
            here, there = gate_up([piece for k in batch for piece in columns[k]], w_gate_up, partner_gate_up)
            for i, k in enumerate(batch):
                own[k] = here[i * rows : (i + 1) * rows]
                other[k] = there[i * rows : (i + 1) * rows]
        halves = [place(part, (rows, units)).reshape(side * rows, units).T for part in (own, other)]
        acts = jnp.zeros((CORES, units, side * rows), jnp.bfloat16)
        acts = lax.dynamic_update_index_in_dim(acts, halves[0], core, 0)
        acts = lax.dynamic_update_index_in_dim(acts, halves[1], 1 - core, 0)
        acts = acts.reshape(CORES * units, side * rows)

        blocks = ring_gather(acts, "x", side, halve=False)
        line = place({k: pieces[0] for k, pieces in blocks.items()}, acts.shape)
        line = line.reshape(side * CORES * units, side * rows)
        partial = [
            lax.dot_general(line, down, (((0,), (1,)), ((), ())), preferred_element_type=jnp.float32)
            for down in (line_down, partner_down)
        ]
        outgoing = jnp.concatenate([p.astype(jnp.bfloat16) for p in partial], axis=1)
        outgoing = outgoing.reshape(side * side, slots, CORES * side * feats)
        arrived = lax.all_to_all(outgoing, ("x", "y"), split_axis=0, concat_axis=0, tiled=True)
        arrived = arrived.reshape(side, side, slots, CORES * side * feats)
        mine = jnp.sum(arrived.astype(jnp.float32), axis=1).astype(jnp.bfloat16)
        mine = mine.reshape(side, slots, CORES, side, feats)
        mine = jnp.where(core == 0, mine, mine[:, :, ::-1])
        mlp_out = mine.transpose(1, 3, 0, 2, 4).reshape(slots, width)

        updated = summed + mlp_out.astype(jnp.float32)
        hidden_out = jnp.where(occupied, updated, 0.0).astype(jnp.bfloat16)
        normed_out = jnp.where(occupied, normalize(updated, next_gain), 0.0).astype(jnp.bfloat16)
        return (hidden_out, normed_out)

    return on_device


def solution(mesh):
    side = math.isqrt(mesh.shape["dp"] // CORES)
    fine = Mesh(mesh.devices.reshape(mesh.shape["groups"], side, side, CORES), ("groups", "y", "x", "core"))
    dp = ("y", "x", "core")
    rows = ("groups",) + dp
    body = build(side)

    return jax.shard_map(
        body,
        mesh=fine,
        in_specs=(P(rows), P(rows, None), P(rows, None), P(), P(None, dp, None), P(None, dp), P()),
        out_specs=(P(rows, None), P(rows, None)),
        check_vma=False,
    )
```

```python
import functools
import math

import jax
import jax.numpy as jnp
from jax import lax
from jax.experimental import pallas as pl
from jax.experimental.pallas import tpu as pltpu
from jax.sharding import Mesh, PartitionSpec as P

EPSILON = 1e-06
CORES = 2
BATCHES = ((0, 1, 7), (2, 6), (3, 5), (4,))


def normalize(values, weight_gain):
    mean_square = jnp.mean(values * values, axis=-1, keepdims=True)
    return values * lax.rsqrt(mean_square + EPSILON) * weight_gain


def gate_up_body(count, *refs):
    blocks, (own, other, own_out, other_out) = refs[:count], refs[count:]
    units = own.shape[1]
    rows = jnp.concatenate([block[...] for block in blocks], axis=0)
    for weights, out in ((own, own_out), (other, other_out)):
        both = weights[...].reshape(2 * units, weights.shape[2])
        both = lax.dot_general(both, rows, (((1,), (1,)), ((), ())), preferred_element_type=jnp.float32)
        gate, up = both[:units], both[units:]
        out[...] = (jax.nn.silu(gate) * up).astype(jnp.bfloat16).T


def hold_body(arrived, out):
    out[...] = arrived[...]


def hold_body_line(arrived, out):
    out[0] = arrived[...]


def hold(arrived):
    block = pl.BlockSpec((1, arrived.shape[1] // 2, arrived.shape[2]), lambda i: (i // 2, i % 2, 0))
    return pl.pallas_call(
        hold_body,
        grid=(2 * arrived.shape[0],),
        in_specs=[block],
        out_specs=block,
        out_shape=jax.ShapeDtypeStruct(arrived.shape, arrived.dtype),
        name="hold",
    )(arrived)


def norm_body(attn, residual, gain, out):
    summed = residual[...].astype(jnp.float32) + attn[...].astype(jnp.float32)
    normed = normalize(summed, gain[...]).astype(jnp.bfloat16)
    for i in range(out.shape[0]):
        out[i] = normed


def norm_rows(attn, residual, gain, copies):
    whole = pl.BlockSpec(memory_space=pltpu.VMEM)
    return pl.pallas_call(
        norm_body,
        in_specs=[whole] * 3,
        out_specs=whole,
        out_shape=jax.ShapeDtypeStruct((copies,) + attn.shape, jnp.bfloat16),
        name="norm_rows",
    )(attn, residual, gain.reshape(1, -1))


def split_lines(weights, lines):
    feats, units = weights.shape
    units //= lines
    return pl.pallas_call(
        hold_body_line,
        grid=(lines,),
        in_specs=[pl.BlockSpec((feats, units), lambda i: (0, i))],
        out_specs=pl.BlockSpec((1, feats, units), lambda i: (i, 0, 0)),
        out_shape=jax.ShapeDtypeStruct((lines, feats, units), weights.dtype),
        name="split_lines",
    )(weights)


def gate_up(blocks, own, other):
    units, width = own.shape[1:]
    rows = sum(block.shape[0] for block in blocks)
    whole = pl.BlockSpec(memory_space=pltpu.VMEM)
    shape = jax.ShapeDtypeStruct((rows, units), jnp.bfloat16)
    return pl.pallas_call(
        functools.partial(gate_up_body, len(blocks)),
        in_specs=[whole] * (len(blocks) + 2),
        out_specs=(whole, whole),
        out_shape=(shape, shape),
        compiler_params=pltpu.CompilerParams(vmem_limit_bytes=24 * 1024 * 1024),
        cost_estimate=pl.CostEstimate(
            flops=8 * rows * units * width, bytes_accessed=8 * units * width + 2 * rows * width, transcendentals=0
        ),
        name="gate_up",
    )(*blocks, own, other)


def shift(extent, by):
    return [(i, (i + by) % extent) for i in range(extent)]


def ring_gather(pieces, axis, extent):
    def send(way, value):
        return lax.ppermute(value, axis, shift(extent, 1 if way == "a" else -1))

    found = {0: list(pieces)}
    ahead, back = list(pieces), list(pieces)
    for hop in range(1, extent // 2):
        for piece in range(2):
            ahead[piece] = send("a", ahead[piece])
            back[piece] = send("b", back[piece])
        found[hop], found[extent - hop] = list(ahead), list(back)
    hop = extent // 2
    found[hop] = [send("a", ahead[0]), send("b", back[1])]
    return found


def ring_gather_whole(block, axis, extent):
    found = {0: block}
    ahead = back = block
    for hop in range(1, extent // 2 + 1):
        ahead = lax.ppermute(ahead, axis, shift(extent, 1))
        found[hop] = ahead
        if hop < extent - hop:
            back = lax.ppermute(back, axis, shift(extent, -1))
            found[extent - hop] = back
    return found


def build(side):
    def on_device(batch_counts, attn_out, residual_in, norm_gain, w_gate_up, w_down, next_gain):
        slots, width = attn_out.shape
        units = w_gate_up.shape[1]
        feats = w_down.shape[1]
        x_at = lax.axis_index("x")
        core = lax.axis_index("core")
        swap = [(0, 1), (1, 0)]

        partner_gate_up = lax.ppermute(w_gate_up, "core", swap)

        occupied = lax.broadcasted_iota(jnp.int32, (slots, 1), 0) < batch_counts[0]
        summed = residual_in.astype(jnp.float32) + attn_out.astype(jnp.float32)

        sent = norm_rows(attn_out, residual_in, norm_gain, side)
        column = lax.all_to_all(sent, "y", split_axis=0, concat_axis=0, tiled=True)
        partner_gate_up = hold(partner_gate_up)
        by_line = split_lines(w_down.T, side)
        column = column.reshape(side * slots, width)

        line_down = lax.all_to_all(by_line, "y", split_axis=0, concat_axis=0, tiled=True)
        line_down = line_down.reshape(side * feats, side * CORES * units)
        partner_down = lax.ppermute(line_down, "core", swap)

        def place(blocks, shape):
            whole = jnp.zeros((side,) + shape, jnp.bfloat16)
            for k in range(side):
                whole = lax.dynamic_update_index_in_dim(whole, blocks[k], (x_at - k) % side, 0)
            return whole

        rows = side * slots
        columns = ring_gather((column[: rows // 2], column[rows // 2 :]), "x", side)
        own, other = {}, {}
        for batch in BATCHES:
            here, there = gate_up([piece for k in batch for piece in columns[k]], w_gate_up, partner_gate_up)
            for i, k in enumerate(batch):
                own[k] = here[i * rows : (i + 1) * rows]
                other[k] = there[i * rows : (i + 1) * rows]
        halves = [place(part, (rows, units)).reshape(side * rows, units).T for part in (own, other)]
        acts = jnp.zeros((CORES, units, side * rows), jnp.bfloat16)
        acts = lax.dynamic_update_index_in_dim(acts, halves[0], core, 0)
        acts = lax.dynamic_update_index_in_dim(acts, halves[1], 1 - core, 0)
        acts = acts.reshape(CORES * units, side * rows)

        line = place(ring_gather_whole(acts, "x", side), acts.shape)
        line = line.reshape(side * CORES * units, side * rows)
        partial = [
            lax.dot_general(line, down, (((0,), (1,)), ((), ())), preferred_element_type=jnp.float32)
            for down in (line_down, partner_down)
        ]
        outgoing = jnp.concatenate([p.astype(jnp.bfloat16) for p in partial], axis=1)
        outgoing = outgoing.reshape(side * side, slots, CORES * side * feats)
        arrived = lax.all_to_all(outgoing, ("x", "y"), split_axis=0, concat_axis=0, tiled=True)
        arrived = arrived.reshape(side, side, slots, CORES * side * feats)
        mine = jnp.sum(arrived.astype(jnp.float32), axis=1).astype(jnp.bfloat16)
        mine = mine.reshape(side, slots, CORES, side, feats)
        mine = jnp.where(core == 0, mine, mine[:, :, ::-1])
        mlp_out = mine.transpose(1, 3, 0, 2, 4).reshape(slots, width)

        updated = summed + mlp_out.astype(jnp.float32)
        hidden_out = jnp.where(occupied, updated, 0.0).astype(jnp.bfloat16)
        normed_out = jnp.where(occupied, normalize(updated, next_gain), 0.0).astype(jnp.bfloat16)
        return (hidden_out, normed_out)

    return on_device


def solution(mesh):
    side = math.isqrt(mesh.shape["dp"] // CORES)
    fine = Mesh(mesh.devices.reshape(mesh.shape["groups"], side, side, CORES), ("groups", "y", "x", "core"))
    dp = ("y", "x", "core")
    rows = ("groups",) + dp
    body = build(side)

    return jax.shard_map(
        body,
        mesh=fine,
        in_specs=(P(rows), P(rows, None), P(rows, None), P(), P(None, dp, None), P(None, dp), P()),
        out_specs=(P(rows, None), P(rows, None)),
        check_vma=False,
    )
```

```python
import functools
import math

import jax
import jax.numpy as jnp
from jax import lax
from jax.experimental import pallas as pl
from jax.experimental.pallas import tpu as pltpu
from jax.sharding import Mesh, PartitionSpec as P

EPSILON = 1e-06
CORES = 2
MIB = 1024 * 1024
BATCHES = ((0, 1, 7), (2, 6), (3, 5), (4,))


def normalize(values, weight_gain):
    mean_square = jnp.mean(values * values, axis=-1, keepdims=True)
    return values * lax.rsqrt(mean_square + EPSILON) * weight_gain


def gate_up_body(count, *refs):
    blocks, (own, other, own_out, other_out) = refs[:count], refs[count:]
    units = own.shape[1]
    rows = jnp.concatenate([block[...] for block in blocks], axis=0)
    for weights, out in ((own, own_out), (other, other_out)):
        both = weights[...].reshape(2 * units, weights.shape[2])
        both = lax.dot_general(both, rows, (((1,), (1,)), ((), ())), preferred_element_type=jnp.float32)
        gate, up = both[:units], both[units:]
        out[...] = (jax.nn.silu(gate) * up).astype(jnp.bfloat16).T


def hold_body(arrived, out):
    out[...] = arrived[...]


def hold_body_line(arrived, out):
    out[0] = arrived[...]


def hold(arrived):
    block = pl.BlockSpec((1, arrived.shape[1] // 2, arrived.shape[2]), lambda i: (i // 2, i % 2, 0))
    return pl.pallas_call(
        hold_body,
        grid=(2 * arrived.shape[0],),
        in_specs=[block],
        out_specs=block,
        out_shape=jax.ShapeDtypeStruct(arrived.shape, arrived.dtype),
        name="hold",
    )(arrived)


def norm_body(attn, residual, gain, out):
    summed = residual[...].astype(jnp.float32) + attn[...].astype(jnp.float32)
    normed = normalize(summed, gain[...]).astype(jnp.bfloat16)
    for i in range(out.shape[0]):
        out[i] = normed


def norm_rows(attn, residual, gain, copies):
    whole = pl.BlockSpec(memory_space=pltpu.VMEM)
    return pl.pallas_call(
        norm_body,
        in_specs=[whole] * 3,
        out_specs=whole,
        out_shape=jax.ShapeDtypeStruct((copies,) + attn.shape, jnp.bfloat16),
        name="norm_rows",
    )(attn, residual, gain.reshape(1, -1))


def split_lines(weights, lines):
    feats, units = weights.shape
    units //= lines
    return pl.pallas_call(
        hold_body_line,
        grid=(lines,),
        in_specs=[pl.BlockSpec((feats, units), lambda i: (0, i))],
        out_specs=pl.BlockSpec((1, feats, units), lambda i: (i, 0, 0)),
        out_shape=jax.ShapeDtypeStruct((lines, feats, units), weights.dtype),
        name="split_lines",
    )(weights)


def gate_up(blocks, own, other):
    units, width = own.shape[1:]
    rows = sum(block.shape[0] for block in blocks)
    whole = pl.BlockSpec(memory_space=pltpu.VMEM)
    shape = jax.ShapeDtypeStruct((rows, units), jnp.bfloat16)
    return pl.pallas_call(
        functools.partial(gate_up_body, len(blocks)),
        in_specs=[whole] * (len(blocks) + 2),
        out_specs=(whole, whole),
        out_shape=(shape, shape),
        compiler_params=pltpu.CompilerParams(vmem_limit_bytes=12 * MIB),
        cost_estimate=pl.CostEstimate(
            flops=8 * rows * units * width, bytes_accessed=8 * units * width + 2 * rows * width, transcendentals=0
        ),
        name="gate_up",
    )(*blocks, own, other)


def down_body(offsets, *refs):
    at, blocks, (own, other, out, line) = refs[0][0], refs[1:-4], refs[-4:]
    side = max(offsets) + 1
    done = [0] * side
    for k, block in zip(offsets, blocks):
        units = line.shape[0] // side
        begin = (at + side - k) % side * units + done[k]
        line[pl.ds(pl.multiple_of(begin, 16), block.shape[0])] = block[...]
        done[k] += block.shape[0]
    both = jnp.concatenate([own[...], other[...]], axis=0)
    sums = jnp.dot(both, line[...], preferred_element_type=jnp.float32).T
    slots = out.shape[1]
    for i in range(out.shape[0]):
        out[i] = sums[i * slots : (i + 1) * slots].astype(jnp.bfloat16)


def down_rows(blocks, at, own, other, slots):
    offsets = [k for k in sorted(blocks) for _ in blocks[k]]
    flat = [piece for k in sorted(blocks) for piece in blocks[k]]
    rows = flat[0].shape[1]
    feats, units = own.shape
    whole = pl.BlockSpec(memory_space=pltpu.VMEM)
    return pl.pallas_call(
        functools.partial(down_body, offsets),
        in_specs=[pl.BlockSpec(memory_space=pltpu.SMEM)] + [whole] * (len(flat) + 2),
        out_specs=whole,
        out_shape=jax.ShapeDtypeStruct((rows // slots, slots, 2 * feats), jnp.bfloat16),
        scratch_shapes=[pltpu.VMEM((units, rows), jnp.bfloat16)],
        compiler_params=pltpu.CompilerParams(vmem_limit_bytes=16 * MIB),
        name="down_rows",
    )(at, *flat, own, other)


def shift(extent, by):
    return [(i, (i + by) % extent) for i in range(extent)]


def ring_gather(block, axis, extent):
    found = {0: [block]}
    ahead = back = block
    for hop in range(1, extent // 2):
        ahead = lax.ppermute(ahead, axis, shift(extent, 1))
        back = lax.ppermute(back, axis, shift(extent, -1))
        found[hop], found[extent - hop] = [ahead], [back]
    hop = extent // 2
    half = block.shape[0] // 2
    ahead = lax.ppermute(ahead[:half], axis, shift(extent, 1))
    back = lax.ppermute(back[half:], axis, shift(extent, -1))
    found[hop] = [ahead, back]
    return found


def build(side):
    def on_device(batch_counts, attn_out, residual_in, norm_gain, w_gate_up, w_down, next_gain):
        slots, width = attn_out.shape
        units = w_gate_up.shape[1]
        feats = w_down.shape[1]
        x_at = lax.axis_index("x")
        core = lax.axis_index("core")
        swap = [(0, 1), (1, 0)]

        partner_gate_up = lax.ppermute(w_gate_up, "core", swap)

        occupied = lax.broadcasted_iota(jnp.int32, (slots, 1), 0) < batch_counts[0]
        summed = residual_in.astype(jnp.float32) + attn_out.astype(jnp.float32)

        sent = norm_rows(attn_out, residual_in, norm_gain, side)
        column = lax.all_to_all(sent, "y", split_axis=0, concat_axis=0, tiled=True)
        partner_gate_up = hold(partner_gate_up)
        by_line = split_lines(w_down.T, side)
        column = column.reshape(side * slots, width)

        line_down = lax.all_to_all(by_line, "y", split_axis=0, concat_axis=0, tiled=True)
        line_down = line_down.reshape(side * feats, side * CORES * units)
        partner_down = lax.ppermute(line_down, "core", swap)

        def place(blocks, shape):
            whole = jnp.zeros((side,) + shape, jnp.bfloat16)
            for k in range(side):
                whole = lax.dynamic_update_index_in_dim(whole, blocks[k], (x_at - k) % side, 0)
            return whole

        rows = side * slots
        columns = ring_gather(column, "x", side)
        own, other = {}, {}
        for batch in BATCHES:
            here, there = gate_up([piece for k in batch for piece in columns[k]], w_gate_up, partner_gate_up)
            for i, k in enumerate(batch):
                own[k] = here[i * rows : (i + 1) * rows]
                other[k] = there[i * rows : (i + 1) * rows]
        halves = [place(part, (rows, units)).reshape(side * rows, units).T for part in (own, other)]
        acts = jnp.zeros((CORES, units, side * rows), jnp.bfloat16)
        acts = lax.dynamic_update_index_in_dim(acts, halves[0], core, 0)
        acts = lax.dynamic_update_index_in_dim(acts, halves[1], 1 - core, 0)
        acts = acts.reshape(CORES * units, side * rows)

        blocks = ring_gather(acts, "x", side)
        outgoing = down_rows(blocks, x_at.reshape(1).astype(jnp.int32), line_down, partner_down, slots)
        arrived = lax.all_to_all(outgoing, ("x", "y"), split_axis=0, concat_axis=0, tiled=True)
        arrived = arrived.reshape(side, side, slots, CORES * side * feats)
        mine = jnp.sum(arrived.astype(jnp.float32), axis=1).astype(jnp.bfloat16)
        mine = mine.reshape(side, slots, CORES, side, feats)
        mine = jnp.where(core == 0, mine, mine[:, :, ::-1])
        mlp_out = mine.transpose(1, 3, 0, 2, 4).reshape(slots, width)

        updated = summed + mlp_out.astype(jnp.float32)
        hidden_out = jnp.where(occupied, updated, 0.0).astype(jnp.bfloat16)
        normed_out = jnp.where(occupied, normalize(updated, next_gain), 0.0).astype(jnp.bfloat16)
        return (hidden_out, normed_out)

    return on_device


def solution(mesh):
    side = math.isqrt(mesh.shape["dp"] // CORES)
    fine = Mesh(mesh.devices.reshape(mesh.shape["groups"], side, side, CORES), ("groups", "y", "x", "core"))
    dp = ("y", "x", "core")
    rows = ("groups",) + dp
    body = build(side)

    return jax.shard_map(
        body,
        mesh=fine,
        in_specs=(P(rows), P(rows, None), P(rows, None), P(), P(None, dp, None), P(None, dp), P()),
        out_specs=(P(rows, None), P(rows, None)),
        check_vma=False,
    )
```

```python
import functools
import math

import jax
import jax.numpy as jnp
from jax import lax
from jax.experimental import pallas as pl
from jax.experimental.pallas import tpu as pltpu
from jax.sharding import Mesh, PartitionSpec as P

EPSILON = 1e-06
CORES = 2
MIB = 1024 * 1024
BATCHES = ((0, 1, 7), (2, 6), (3, 5), (4,))


def normalize(values, weight_gain):
    mean_square = jnp.mean(values * values, axis=-1, keepdims=True)
    return values * lax.rsqrt(mean_square + EPSILON) * weight_gain


def gate_up_body(count, *refs):
    blocks, (own, other, own_out, other_out) = refs[:count], refs[count:]
    units = own.shape[1]
    rows = jnp.concatenate([block[...] for block in blocks], axis=0)
    for weights, out in ((own, own_out), (other, other_out)):
        both = weights[...].reshape(2 * units, weights.shape[2])
        both = lax.dot_general(both, rows, (((1,), (1,)), ((), ())), preferred_element_type=jnp.float32)
        gate, up = both[:units], both[units:]
        out[...] = (jax.nn.silu(gate) * up).astype(jnp.bfloat16).T


def hold_body(arrived, out):
    out[...] = arrived[...]


def hold_body_line(arrived, out):
    out[0] = arrived[...]


def hold(arrived):
    block = pl.BlockSpec((1, arrived.shape[1] // 2, arrived.shape[2]), lambda i: (i // 2, i % 2, 0))
    return pl.pallas_call(
        hold_body,
        grid=(2 * arrived.shape[0],),
        in_specs=[block],
        out_specs=block,
        out_shape=jax.ShapeDtypeStruct(arrived.shape, arrived.dtype),
        name="hold",
    )(arrived)


def norm_body(attn, residual, gain, out):
    summed = residual[...].astype(jnp.float32) + attn[...].astype(jnp.float32)
    normed = normalize(summed, gain[...]).astype(jnp.bfloat16)
    for i in range(out.shape[0]):
        out[i] = normed


def norm_rows(attn, residual, gain, copies):
    whole = pl.BlockSpec(memory_space=pltpu.VMEM)
    return pl.pallas_call(
        norm_body,
        in_specs=[whole] * 3,
        out_specs=whole,
        out_shape=jax.ShapeDtypeStruct((copies,) + attn.shape, jnp.bfloat16),
        name="norm_rows",
    )(attn, residual, gain.reshape(1, -1))


def split_lines(weights, lines):
    feats, units = weights.shape
    units //= lines
    return pl.pallas_call(
        hold_body_line,
        grid=(lines,),
        in_specs=[pl.BlockSpec((feats, units), lambda i: (0, i))],
        out_specs=pl.BlockSpec((1, feats, units), lambda i: (i, 0, 0)),
        out_shape=jax.ShapeDtypeStruct((lines, feats, units), weights.dtype),
        name="split_lines",
    )(weights)


def gate_up(blocks, own, other):
    units, width = own.shape[1:]
    rows = sum(block.shape[0] for block in blocks)
    whole = pl.BlockSpec(memory_space=pltpu.VMEM)
    shape = jax.ShapeDtypeStruct((rows, units), jnp.bfloat16)
    return pl.pallas_call(
        functools.partial(gate_up_body, len(blocks)),
        in_specs=[whole] * (len(blocks) + 2),
        out_specs=(whole, whole),
        out_shape=(shape, shape),
        compiler_params=pltpu.CompilerParams(vmem_limit_bytes=12 * MIB),
        cost_estimate=pl.CostEstimate(
            flops=8 * rows * units * width, bytes_accessed=8 * units * width + 2 * rows * width, transcendentals=0
        ),
        name="gate_up",
    )(*blocks, own, other)


def place_of(x_at, core, k, side):
    return (x_at[0] + side - k + 2 * k * core[0]) % side


def place_body(batches, x_at, core, *refs):
    parts, (out, whole) = refs[:-2], refs[-2:]
    rows = parts[0].shape[0] // len(batches[0])
    side = whole.shape[0] // rows
    for i in range(2):
        for batch, part in zip(batches, parts[i::2]):
            for j, k in enumerate(batch):
                begin = pl.multiple_of(place_of(x_at, core, k, side) * rows, rows)
                whole[pl.ds(begin, rows)] = part[j * rows : (j + 1) * rows]
        out[(core[0] + i) % 2] = whole[...].T


def place_acts(parts, x_at, core):
    units = parts[0].shape[1]
    rows = sum(part.shape[0] for part in parts[::2])
    whole = pl.BlockSpec(memory_space=pltpu.VMEM)
    return pl.pallas_call(
        functools.partial(place_body, BATCHES),
        in_specs=[pl.BlockSpec(memory_space=pltpu.SMEM)] * 2 + [whole] * len(parts),
        out_specs=whole,
        out_shape=jax.ShapeDtypeStruct((2, units, rows), jnp.bfloat16),
        scratch_shapes=[pltpu.VMEM((rows, units), jnp.bfloat16)],
        compiler_params=pltpu.CompilerParams(vmem_limit_bytes=4 * MIB),
        name="place_acts",
    )(x_at, core, *parts)


def down_body(offsets, *refs):
    (x_at, core), blocks, (own, other, out, line) = refs[:2], refs[2:-4], refs[-4:]
    side = max(offsets) + 1
    done = [0] * side
    for k, block in zip(offsets, blocks):
        units = line.shape[0] // side
        begin = place_of(x_at, core, k, side) * units + done[k]
        line[pl.ds(pl.multiple_of(begin, 16), block.shape[0])] = block[...]
        done[k] += block.shape[0]
    both = jnp.concatenate([own[...], other[...]], axis=0)
    sums = jnp.dot(both, line[...], preferred_element_type=jnp.float32).T
    slots = out.shape[1]
    for i in range(out.shape[0]):
        out[i] = sums[i * slots : (i + 1) * slots].astype(jnp.bfloat16)


def down_rows(blocks, x_at, core, own, other, slots):
    offsets = [k for k in sorted(blocks) for _ in blocks[k]]
    flat = [piece for k in sorted(blocks) for piece in blocks[k]]
    rows = flat[0].shape[1]
    feats, units = own.shape
    whole = pl.BlockSpec(memory_space=pltpu.VMEM)
    return pl.pallas_call(
        functools.partial(down_body, offsets),
        in_specs=[pl.BlockSpec(memory_space=pltpu.SMEM)] * 2 + [whole] * (len(flat) + 2),
        out_specs=whole,
        out_shape=jax.ShapeDtypeStruct((rows // slots, slots, 2 * feats), jnp.bfloat16),
        scratch_shapes=[pltpu.VMEM((units, rows), jnp.bfloat16)],
        compiler_params=pltpu.CompilerParams(vmem_limit_bytes=16 * MIB),
        name="down_rows",
    )(x_at, core, *flat, own, other)


def opposed(extent, way):
    pairs = []
    for at in range(extent):
        for core, step in enumerate((1, -1) if way == "a" else (-1, 1)):
            pairs.append((at * CORES + core, (at + step) % extent * CORES + core))
    return pairs


def ring_gather(block, extent):
    def send(value, way):
        return lax.ppermute(value, ("x", "core"), opposed(extent, way))

    found = {0: [block]}
    ahead = back = block
    for hop in range(1, extent // 2):
        ahead, back = send(ahead, "a"), send(back, "b")
        found[hop], found[extent - hop] = [ahead], [back]
    found[extent // 2] = [send(ahead, "a")]
    return found


def build(side):
    def on_device(batch_counts, attn_out, residual_in, norm_gain, w_gate_up, w_down, next_gain):
        slots, width = attn_out.shape
        units = w_gate_up.shape[1]
        feats = w_down.shape[1]
        x_at = lax.axis_index("x")
        core = lax.axis_index("core")
        swap = [(0, 1), (1, 0)]

        partner_gate_up = lax.ppermute(w_gate_up, "core", swap)

        occupied = lax.broadcasted_iota(jnp.int32, (slots, 1), 0) < batch_counts[0]
        summed = residual_in.astype(jnp.float32) + attn_out.astype(jnp.float32)

        sent = norm_rows(attn_out, residual_in, norm_gain, side)
        at = (x_at.reshape(1).astype(jnp.int32), core.reshape(1).astype(jnp.int32))
        sent, at = lax.optimization_barrier((sent, at))
        column = lax.all_to_all(sent, "y", split_axis=0, concat_axis=0, tiled=True)
        partner_gate_up = hold(partner_gate_up)
        by_line = split_lines(w_down.T, side)
        column = column.reshape(side * slots, width)

        line_down = lax.all_to_all(by_line, "y", split_axis=0, concat_axis=0, tiled=True)
        line_down = line_down.reshape(side * feats, side * CORES * units)
        partner_down = lax.ppermute(line_down, "core", swap)

        rows = side * slots
        columns = ring_gather(column, side)
        parts = []
        for batch in BATCHES:
            parts += gate_up([piece for k in batch for piece in columns[k]], w_gate_up, partner_gate_up)
        acts = place_acts(parts, *at).reshape(CORES * units, side * rows)

        blocks = ring_gather(acts, side)
        outgoing = down_rows(blocks, *at, line_down, partner_down, slots)
        arrived = lax.all_to_all(outgoing, ("x", "y"), split_axis=0, concat_axis=0, tiled=True)
        arrived = arrived.reshape(side, side, slots, CORES * side * feats)
        mine = jnp.sum(arrived.astype(jnp.float32), axis=1).astype(jnp.bfloat16)
        mine = mine.reshape(side, slots, CORES, side, feats)
        mine = jnp.where(core == 0, mine, mine[:, :, ::-1])
        mlp_out = mine.transpose(1, 3, 0, 2, 4).reshape(slots, width)

        updated = summed + mlp_out.astype(jnp.float32)
        hidden_out = jnp.where(occupied, updated, 0.0).astype(jnp.bfloat16)
        normed_out = jnp.where(occupied, normalize(updated, next_gain), 0.0).astype(jnp.bfloat16)
        return (hidden_out, normed_out)

    return on_device


def solution(mesh):
    side = math.isqrt(mesh.shape["dp"] // CORES)
    fine = Mesh(mesh.devices.reshape(mesh.shape["groups"], side, side, CORES), ("groups", "y", "x", "core"))
    dp = ("y", "x", "core")
    rows = ("groups",) + dp
    body = build(side)

    return jax.shard_map(
        body,
        mesh=fine,
        in_specs=(P(rows), P(rows, None), P(rows, None), P(), P(None, dp, None), P(None, dp), P()),
        out_specs=(P(rows, None), P(rows, None)),
        check_vma=False,
    )
```

```python
import functools
import math

import jax
import jax.numpy as jnp
from jax import lax
from jax.experimental import pallas as pl
from jax.experimental.pallas import tpu as pltpu
from jax.sharding import Mesh, PartitionSpec as P

EPSILON = 1e-06
CORES = 2
MIB = 1024 * 1024
BATCHES = ((0, 1, 7), (2, 6), (3, 5), (4,))


def normalize(values, weight_gain):
    mean_square = jnp.mean(values * values, axis=-1, keepdims=True)
    return values * lax.rsqrt(mean_square + EPSILON) * weight_gain


def gate_up_body(count, *refs):
    blocks, (own, other, own_out, other_out) = refs[:count], refs[count:]
    units = own.shape[1]
    rows = jnp.concatenate([block[...] for block in blocks], axis=0)
    for weights, out in ((own, own_out), (other, other_out)):
        both = weights[...].reshape(2 * units, weights.shape[2])
        both = lax.dot_general(both, rows, (((1,), (1,)), ((), ())), preferred_element_type=jnp.float32)
        gate, up = both[:units], both[units:]
        out[...] = (jax.nn.silu(gate) * up).astype(jnp.bfloat16).T


def hold_body(arrived, out):
    out[...] = arrived[...]


def hold_body_line(arrived, out):
    out[0] = arrived[...]


def hold(arrived):
    block = pl.BlockSpec((1, arrived.shape[1] // 2, arrived.shape[2]), lambda i: (i // 2, i % 2, 0))
    return pl.pallas_call(
        hold_body,
        grid=(2 * arrived.shape[0],),
        in_specs=[block],
        out_specs=block,
        out_shape=jax.ShapeDtypeStruct(arrived.shape, arrived.dtype),
        name="hold",
    )(arrived)


def norm_body(attn, residual, gain, out):
    summed = residual[...].astype(jnp.float32) + attn[...].astype(jnp.float32)
    normed = normalize(summed, gain[...]).astype(jnp.bfloat16)
    for i in range(out.shape[0]):
        out[i] = normed


def norm_rows(attn, residual, gain, copies):
    whole = pl.BlockSpec(memory_space=pltpu.VMEM)
    return pl.pallas_call(
        norm_body,
        in_specs=[whole] * 3,
        out_specs=whole,
        out_shape=jax.ShapeDtypeStruct((copies,) + attn.shape, jnp.bfloat16),
        name="norm_rows",
    )(attn, residual, gain.reshape(1, -1))


def split_lines(weights, lines):
    feats, units = weights.shape
    units //= lines
    return pl.pallas_call(
        hold_body_line,
        grid=(lines,),
        in_specs=[pl.BlockSpec((feats, units), lambda i: (0, i))],
        out_specs=pl.BlockSpec((1, feats, units), lambda i: (i, 0, 0)),
        out_shape=jax.ShapeDtypeStruct((lines, feats, units), weights.dtype),
        name="split_lines",
    )(weights)


def gate_up(blocks, own, other):
    units, width = own.shape[1:]
    rows = sum(block.shape[0] for block in blocks)
    whole = pl.BlockSpec(memory_space=pltpu.VMEM)
    shape = jax.ShapeDtypeStruct((rows, units), jnp.bfloat16)
    return pl.pallas_call(
        functools.partial(gate_up_body, len(blocks)),
        in_specs=[whole] * (len(blocks) + 2),
        out_specs=(whole, whole),
        out_shape=(shape, shape),
        compiler_params=pltpu.CompilerParams(vmem_limit_bytes=12 * MIB),
        cost_estimate=pl.CostEstimate(
            flops=8 * rows * units * width, bytes_accessed=8 * units * width + 2 * rows * width, transcendentals=0
        ),
        name="gate_up",
    )(*blocks, own, other)


def place_body(batches, x_at, core, *refs):
    parts, (first, second, whole) = refs[:-3], refs[-3:]
    rows = parts[0].shape[0] // len(batches[0])
    side = whole.shape[1] // rows
    for i in range(2):
        for batch, part in zip(batches, parts[i::2]):
            for j, k in enumerate(batch):
                begin = pl.multiple_of((x_at[0] + side - k) % side * rows, rows)
                whole[(core[0] + i) % 2, pl.ds(begin, rows)] = part[j * rows : (j + 1) * rows]
    first[...] = whole[0].T
    second[...] = whole[1].T


def place_acts(parts, x_at, core):
    units = parts[0].shape[1]
    rows = sum(part.shape[0] for part in parts[::2])
    whole = pl.BlockSpec(memory_space=pltpu.VMEM)
    return pl.pallas_call(
        functools.partial(place_body, BATCHES),
        in_specs=[pl.BlockSpec(memory_space=pltpu.SMEM)] * 2 + [whole] * len(parts),
        out_specs=(whole, whole),
        out_shape=(jax.ShapeDtypeStruct((units, rows), jnp.bfloat16),) * 2,
        scratch_shapes=[pltpu.VMEM((2, rows, units), jnp.bfloat16)],
        compiler_params=pltpu.CompilerParams(vmem_limit_bytes=4 * MIB),
        name="place_acts",
    )(x_at, core, *parts)


def down_body(offsets, *refs):
    x_at, blocks, (own, other, out, line) = refs[0], refs[1:-4], refs[-4:]
    side = max(offsets) + 1
    done = [0] * side
    for k, block in zip(offsets, blocks):
        units = line.shape[0] // side
        begin = (x_at[0] + side - k) % side * units + done[k]
        line[pl.ds(pl.multiple_of(begin, 16), block.shape[0])] = block[...]
        done[k] += block.shape[0]
    both = jnp.concatenate([own[...], other[...]], axis=0)
    sums = jnp.dot(both, line[...], preferred_element_type=jnp.float32).T
    slots = out.shape[1]
    for i in range(out.shape[0]):
        out[i] = sums[i * slots : (i + 1) * slots].astype(jnp.bfloat16)


def down_rows(blocks, x_at, own, other, slots):
    offsets = [k for k in sorted(blocks) for _ in blocks[k]]
    flat = [piece for k in sorted(blocks) for piece in blocks[k]]
    rows = flat[0].shape[1]
    feats, units = own.shape
    whole = pl.BlockSpec(memory_space=pltpu.VMEM)
    return pl.pallas_call(
        functools.partial(down_body, offsets),
        in_specs=[pl.BlockSpec(memory_space=pltpu.SMEM)] + [whole] * (len(flat) + 2),
        out_specs=whole,
        out_shape=jax.ShapeDtypeStruct((rows // slots, slots, 2 * feats), jnp.bfloat16),
        scratch_shapes=[pltpu.VMEM((units, rows), jnp.bfloat16)],
        compiler_params=pltpu.CompilerParams(vmem_limit_bytes=16 * MIB),
        name="down_rows",
    )(x_at, *flat, own, other)


def shift(extent, by):
    return [(i, (i + by) % extent) for i in range(extent)]


def ring_gather(pieces, extent):
    def send(value, way):
        return lax.ppermute(value, "x", shift(extent, 1 if way == "a" else -1))

    found = {0: list(pieces)}
    ahead, back = list(pieces), list(pieces)
    for hop in range(1, extent // 2):
        for i in range(len(pieces)):
            ahead[i], back[i] = send(ahead[i], "a"), send(back[i], "b")
        found[hop], found[extent - hop] = list(ahead), list(back)
    if len(pieces) == 1:
        half = pieces[0].shape[0] // 2
        ahead, back = [ahead[0][:half]], [back[0][half:]]
    hop = extent // 2
    found[hop] = [send(ahead[0], "a"), send(back[-1], "b")]
    return found


def build(side):
    def on_device(batch_counts, attn_out, residual_in, norm_gain, w_gate_up, w_down, next_gain):
        slots, width = attn_out.shape
        units = w_gate_up.shape[1]
        feats = w_down.shape[1]
        x_at = lax.axis_index("x")
        core = lax.axis_index("core")
        swap = [(0, 1), (1, 0)]

        partner_gate_up = lax.ppermute(w_gate_up, "core", swap)

        occupied = lax.broadcasted_iota(jnp.int32, (slots, 1), 0) < batch_counts[0]
        summed = residual_in.astype(jnp.float32) + attn_out.astype(jnp.float32)

        sent = norm_rows(attn_out, residual_in, norm_gain, side)
        at = (x_at.reshape(1).astype(jnp.int32), core.reshape(1).astype(jnp.int32))
        sent, at = lax.optimization_barrier((sent, at))
        column = lax.all_to_all(sent, "y", split_axis=0, concat_axis=0, tiled=True)
        partner_gate_up = hold(partner_gate_up)
        by_line = split_lines(w_down.T, side)
        column = column.reshape(side * slots, width)

        line_down = lax.all_to_all(by_line, "y", split_axis=0, concat_axis=0, tiled=True)
        line_down = line_down.reshape(side * feats, side * CORES * units)
        partner_down = lax.ppermute(line_down, "core", swap)

        columns = ring_gather([column], side)
        parts = []
        for batch in BATCHES:
            parts += gate_up([piece for k in batch for piece in columns[k]], w_gate_up, partner_gate_up)
        acts = place_acts(parts, *at)

        blocks = ring_gather(acts, side)
        outgoing = down_rows(blocks, at[0], line_down, partner_down, slots)
        arrived = lax.all_to_all(outgoing, ("x", "y"), split_axis=0, concat_axis=0, tiled=True)
        arrived = arrived.reshape(side, side, slots, CORES * side * feats)
        mine = jnp.sum(arrived.astype(jnp.float32), axis=1).astype(jnp.bfloat16)
        mine = mine.reshape(side, slots, CORES, side, feats)
        mine = jnp.where(core == 0, mine, mine[:, :, ::-1])
        mlp_out = mine.transpose(1, 3, 0, 2, 4).reshape(slots, width)

        updated = summed + mlp_out.astype(jnp.float32)
        hidden_out = jnp.where(occupied, updated, 0.0).astype(jnp.bfloat16)
        normed_out = jnp.where(occupied, normalize(updated, next_gain), 0.0).astype(jnp.bfloat16)
        return (hidden_out, normed_out)

    return on_device


def solution(mesh):
    side = math.isqrt(mesh.shape["dp"] // CORES)
    fine = Mesh(mesh.devices.reshape(mesh.shape["groups"], side, side, CORES), ("groups", "y", "x", "core"))
    dp = ("y", "x", "core")
    rows = ("groups",) + dp
    body = build(side)

    return jax.shard_map(
        body,
        mesh=fine,
        in_specs=(P(rows), P(rows, None), P(rows, None), P(), P(None, dp, None), P(None, dp), P()),
        out_specs=(P(rows, None), P(rows, None)),
        check_vma=False,
    )
```

```python
import functools
import math

import jax
import jax.numpy as jnp
from jax import lax
from jax.experimental import pallas as pl
from jax.experimental.pallas import tpu as pltpu
from jax.sharding import Mesh, PartitionSpec as P

EPSILON = 1e-06
CORES = 2
MIB = 1024 * 1024
BATCHES = ((0, 1, 7), (2, 6), (3, 5), (4,))


def normalize(values, weight_gain):
    mean_square = jnp.mean(values * values, axis=-1, keepdims=True)
    return values * lax.rsqrt(mean_square + EPSILON) * weight_gain


def gate_up_body(count, *refs):
    blocks, (own, other, own_out, other_out) = refs[:count], refs[count:]
    units = own.shape[1]
    rows = jnp.concatenate([block[...] for block in blocks], axis=0)
    for weights, out in ((own, own_out), (other, other_out)):
        both = weights[...].reshape(2 * units, weights.shape[2])
        both = lax.dot_general(both, rows, (((1,), (1,)), ((), ())), preferred_element_type=jnp.float32)
        gate, up = both[:units], both[units:]
        out[...] = (jax.nn.silu(gate) * up).astype(jnp.bfloat16).T


def hold_body(arrived, out):
    out[...] = arrived[...]


def hold_body_line(arrived, out):
    out[0] = arrived[...]


def hold(arrived):
    block = pl.BlockSpec((1, arrived.shape[1] // 2, arrived.shape[2]), lambda i: (i // 2, i % 2, 0))
    return pl.pallas_call(
        hold_body,
        grid=(2 * arrived.shape[0],),
        in_specs=[block],
        out_specs=block,
        out_shape=jax.ShapeDtypeStruct(arrived.shape, arrived.dtype),
        name="hold",
    )(arrived)


def norm_body(attn, residual, gain, out):
    summed = residual[...].astype(jnp.float32) + attn[...].astype(jnp.float32)
    normed = normalize(summed, gain[...]).astype(jnp.bfloat16)
    for i in range(out.shape[0]):
        out[i] = normed


def norm_rows(attn, residual, gain, copies):
    whole = pl.BlockSpec(memory_space=pltpu.VMEM)
    return pl.pallas_call(
        norm_body,
        in_specs=[whole] * 3,
        out_specs=whole,
        out_shape=jax.ShapeDtypeStruct((copies,) + attn.shape, jnp.bfloat16),
        name="norm_rows",
    )(attn, residual, gain.reshape(1, -1))


def split_lines(weights, lines):
    feats, units = weights.shape
    units //= lines
    return pl.pallas_call(
        hold_body_line,
        grid=(lines,),
        in_specs=[pl.BlockSpec((feats, units), lambda i: (0, i))],
        out_specs=pl.BlockSpec((1, feats, units), lambda i: (i, 0, 0)),
        out_shape=jax.ShapeDtypeStruct((lines, feats, units), weights.dtype),
        name="split_lines",
    )(weights)


def gate_up(blocks, own, other):
    units, width = own.shape[1:]
    rows = sum(block.shape[0] for block in blocks)
    whole = pl.BlockSpec(memory_space=pltpu.VMEM)
    shape = jax.ShapeDtypeStruct((rows, units), jnp.bfloat16)
    return pl.pallas_call(
        functools.partial(gate_up_body, len(blocks)),
        in_specs=[whole] * (len(blocks) + 2),
        out_specs=(whole, whole),
        out_shape=(shape, shape),
        compiler_params=pltpu.CompilerParams(vmem_limit_bytes=12 * MIB),
        cost_estimate=pl.CostEstimate(
            flops=8 * rows * units * width, bytes_accessed=8 * units * width + 2 * rows * width, transcendentals=0
        ),
        name="gate_up",
    )(*blocks, own, other)


def place_body(batches, x_at, core, *refs):
    parts, (out, whole) = refs[:-2], refs[-2:]
    rows = parts[0].shape[0] // len(batches[0])
    side = whole.shape[0] // rows
    for i in range(2):
        for batch, part in zip(batches, parts[i::2]):
            for j, k in enumerate(batch):
                begin = pl.multiple_of((x_at[0] + side - k) % side * rows, rows)
                whole[pl.ds(begin, rows)] = part[j * rows : (j + 1) * rows]
        out[(core[0] + i) % 2] = whole[...].T


def place_acts(parts, x_at, core):
    units = parts[0].shape[1]
    rows = sum(part.shape[0] for part in parts[::2])
    whole = pl.BlockSpec(memory_space=pltpu.VMEM)
    return pl.pallas_call(
        functools.partial(place_body, BATCHES),
        in_specs=[pl.BlockSpec(memory_space=pltpu.SMEM)] * 2 + [whole] * len(parts),
        out_specs=whole,
        out_shape=jax.ShapeDtypeStruct((2, units, rows), jnp.bfloat16),
        scratch_shapes=[pltpu.VMEM((rows, units), jnp.bfloat16)],
        compiler_params=pltpu.CompilerParams(vmem_limit_bytes=4 * MIB),
        name="place_acts",
    )(x_at, core, *parts)


def down_body(offsets, *refs):
    x_at, blocks, (own, other, out, line) = refs[0], refs[1:-4], refs[-4:]
    side = max(offsets) + 1
    done = [0] * side
    for k, block in zip(offsets, blocks):
        units = line.shape[0] // side
        begin = (x_at[0] + side - k) % side * units + done[k]
        line[pl.ds(pl.multiple_of(begin, 16), block.shape[0])] = block[...]
        done[k] += block.shape[0]
    both = jnp.concatenate([own[...], other[...]], axis=0)
    sums = jnp.dot(both, line[...], preferred_element_type=jnp.float32).T
    slots = out.shape[1]
    for i in range(out.shape[0]):
        out[i] = sums[i * slots : (i + 1) * slots].astype(jnp.bfloat16)


def down_rows(blocks, x_at, own, other, slots):
    offsets = [k for k in sorted(blocks) for _ in blocks[k]]
    flat = [piece for k in sorted(blocks) for piece in blocks[k]]
    rows = flat[0].shape[1]
    feats, units = own.shape
    whole = pl.BlockSpec(memory_space=pltpu.VMEM)
    return pl.pallas_call(
        functools.partial(down_body, offsets),
        in_specs=[pl.BlockSpec(memory_space=pltpu.SMEM)] + [whole] * (len(flat) + 2),
        out_specs=whole,
        out_shape=jax.ShapeDtypeStruct((rows // slots, slots, 2 * feats), jnp.bfloat16),
        scratch_shapes=[pltpu.VMEM((units, rows), jnp.bfloat16)],
        compiler_params=pltpu.CompilerParams(vmem_limit_bytes=16 * MIB),
        name="down_rows",
    )(x_at, *flat, own, other)


def shift(extent, by):
    return [(i, (i + by) % extent) for i in range(extent)]


def ring_gather(block, extent):
    def send(value, way):
        return lax.ppermute(value, "x", shift(extent, 1 if way == "a" else -1))

    found = {0: [block]}
    ahead = back = block
    for hop in range(1, extent // 2):
        ahead, back = send(ahead, "a"), send(back, "b")
        found[hop], found[extent - hop] = [ahead], [back]
    half = block.shape[0] // 2
    hop = extent // 2
    found[hop] = [send(ahead[:half], "a"), send(back[half:], "b")]
    return found


def build(side):
    def on_device(batch_counts, attn_out, residual_in, norm_gain, w_gate_up, w_down, next_gain):
        slots, width = attn_out.shape
        units = w_gate_up.shape[1]
        feats = w_down.shape[1]
        x_at = lax.axis_index("x")
        core = lax.axis_index("core")
        swap = [(0, 1), (1, 0)]

        partner_gate_up = lax.ppermute(w_gate_up, "core", swap)

        occupied = lax.broadcasted_iota(jnp.int32, (slots, 1), 0) < batch_counts[0]
        summed = residual_in.astype(jnp.float32) + attn_out.astype(jnp.float32)

        sent = norm_rows(attn_out, residual_in, norm_gain, side)
        at = (x_at.reshape(1).astype(jnp.int32), core.reshape(1).astype(jnp.int32))
        sent, at = lax.optimization_barrier((sent, at))
        column = lax.all_to_all(sent, "y", split_axis=0, concat_axis=0, tiled=True)
        partner_gate_up = hold(partner_gate_up)
        by_line = split_lines(w_down.T, side)
        column = column.reshape(side * slots, width)

        line_down = lax.all_to_all(by_line, "y", split_axis=0, concat_axis=0, tiled=True)
        line_down = line_down.reshape(side * feats, side * CORES * units)
        partner_down = lax.ppermute(line_down, "core", swap)

        rows = side * slots
        columns = ring_gather(column, side)
        parts = []
        for batch in BATCHES:
            parts += gate_up([piece for k in batch for piece in columns[k]], w_gate_up, partner_gate_up)
        acts = place_acts(parts, *at).reshape(CORES * units, side * rows)

        blocks = ring_gather(acts, side)
        outgoing = down_rows(blocks, at[0], line_down, partner_down, slots)
        arrived = lax.all_to_all(outgoing, ("x", "y"), split_axis=0, concat_axis=0, tiled=True)
        arrived = arrived.reshape(side, side, slots, CORES * side * feats)
        mine = jnp.sum(arrived.astype(jnp.float32), axis=1).astype(jnp.bfloat16)
        mine = mine.reshape(side, slots, CORES, side, feats)
        mine = jnp.where(core == 0, mine, mine[:, :, ::-1])
        mlp_out = mine.transpose(1, 3, 0, 2, 4).reshape(slots, width)

        updated = summed + mlp_out.astype(jnp.float32)
        hidden_out = jnp.where(occupied, updated, 0.0).astype(jnp.bfloat16)
        normed_out = jnp.where(occupied, normalize(updated, next_gain), 0.0).astype(jnp.bfloat16)
        return (hidden_out, normed_out)

    return on_device


def solution(mesh):
    side = math.isqrt(mesh.shape["dp"] // CORES)
    fine = Mesh(mesh.devices.reshape(mesh.shape["groups"], side, side, CORES), ("groups", "y", "x", "core"))
    dp = ("y", "x", "core")
    rows = ("groups",) + dp
    body = build(side)

    return jax.shard_map(
        body,
        mesh=fine,
        in_specs=(P(rows), P(rows, None), P(rows, None), P(), P(None, dp, None), P(None, dp), P()),
        out_specs=(P(rows, None), P(rows, None)),
        check_vma=False,
    )
```

```python
import functools
import math

import jax
import jax.numpy as jnp
from jax import lax
from jax.experimental import pallas as pl
from jax.experimental.pallas import tpu as pltpu
from jax.sharding import Mesh, PartitionSpec as P

EPSILON = 1e-06
CORES = 2
MIB = 1024 * 1024
BATCHES = ((0, 1, 7), (2, 6), (3, 5), (4,))


def normalize(values, weight_gain):
    mean_square = jnp.mean(values * values, axis=-1, keepdims=True)
    return values * lax.rsqrt(mean_square + EPSILON) * weight_gain


def gate_up_body(count, *refs):
    blocks, (own, other, own_out, other_out) = refs[:count], refs[count:]
    units = own.shape[1]
    rows = jnp.concatenate([block[...] for block in blocks], axis=0)
    for weights, out in ((own, own_out), (other, other_out)):
        both = weights[...].reshape(2 * units, weights.shape[2])
        both = lax.dot_general(both, rows, (((1,), (1,)), ((), ())), preferred_element_type=jnp.float32)
        gate, up = both[:units], both[units:]
        out[...] = (jax.nn.silu(gate) * up).astype(jnp.bfloat16).T


def hold_body(arrived, out):
    out[...] = arrived[...]


def hold_body_line(arrived, out):
    out[0] = arrived[...]


def hold(arrived):
    block = pl.BlockSpec((1, arrived.shape[1] // 2, arrived.shape[2]), lambda i: (i // 2, i % 2, 0))
    return pl.pallas_call(
        hold_body,
        grid=(2 * arrived.shape[0],),
        in_specs=[block],
        out_specs=block,
        out_shape=jax.ShapeDtypeStruct(arrived.shape, arrived.dtype),
        name="hold",
    )(arrived)


def norm_body(attn, residual, gain, out):
    summed = residual[...].astype(jnp.float32) + attn[...].astype(jnp.float32)
    normed = normalize(summed, gain[...]).astype(jnp.bfloat16)
    for i in range(out.shape[0]):
        out[i] = normed


def norm_rows(attn, residual, gain, copies):
    whole = pl.BlockSpec(memory_space=pltpu.VMEM)
    return pl.pallas_call(
        norm_body,
        in_specs=[whole] * 3,
        out_specs=whole,
        out_shape=jax.ShapeDtypeStruct((copies,) + attn.shape, jnp.bfloat16),
        name="norm_rows",
    )(attn, residual, gain.reshape(1, -1))


def split_lines(weights, lines):
    feats, units = weights.shape
    units //= lines
    return pl.pallas_call(
        hold_body_line,
        grid=(lines,),
        in_specs=[pl.BlockSpec((feats, units), lambda i: (0, i))],
        out_specs=pl.BlockSpec((1, feats, units), lambda i: (i, 0, 0)),
        out_shape=jax.ShapeDtypeStruct((lines, feats, units), weights.dtype),
        name="split_lines",
    )(weights)


def gate_up(blocks, own, other):
    units, width = own.shape[1:]
    rows = sum(block.shape[0] for block in blocks)
    whole = pl.BlockSpec(memory_space=pltpu.VMEM)
    shape = jax.ShapeDtypeStruct((rows, units), jnp.bfloat16)
    return pl.pallas_call(
        functools.partial(gate_up_body, len(blocks)),
        in_specs=[whole] * (len(blocks) + 2),
        out_specs=(whole, whole),
        out_shape=(shape, shape),
        compiler_params=pltpu.CompilerParams(vmem_limit_bytes=12 * MIB),
        cost_estimate=pl.CostEstimate(
            flops=8 * rows * units * width, bytes_accessed=8 * units * width + 2 * rows * width, transcendentals=0
        ),
        name="gate_up",
    )(*blocks, own, other)


def place_body(batches, x_at, core, *refs):
    parts, (out, whole) = refs[:-2], refs[-2:]
    rows = parts[0].shape[0] // len(batches[0])
    side = whole.shape[0] // rows
    for i in range(2):
        for batch, part in zip(batches, parts[i::2]):
            for j, k in enumerate(batch):
                begin = pl.multiple_of((x_at[0] + side - k) % side * rows, rows)
                whole[pl.ds(begin, rows)] = part[j * rows : (j + 1) * rows]
        out[(core[0] + i) % 2] = whole[...].T


def place_acts(parts, x_at, core):
    units = parts[0].shape[1]
    rows = sum(part.shape[0] for part in parts[::2])
    whole = pl.BlockSpec(memory_space=pltpu.VMEM)
    return pl.pallas_call(
        functools.partial(place_body, BATCHES),
        in_specs=[pl.BlockSpec(memory_space=pltpu.SMEM)] * 2 + [whole] * len(parts),
        out_specs=whole,
        out_shape=jax.ShapeDtypeStruct((2, units, rows), jnp.bfloat16),
        scratch_shapes=[pltpu.VMEM((rows, units), jnp.bfloat16)],
        compiler_params=pltpu.CompilerParams(vmem_limit_bytes=4 * MIB),
        name="place_acts",
    )(x_at, core, *parts)


def down_body(offsets, *refs):
    x_at, blocks, (own, other, out, line) = refs[0], refs[1:-4], refs[-4:]
    side = max(offsets) + 1
    done = [0] * side
    for k, block in zip(offsets, blocks):
        units = line.shape[0] // side
        begin = (x_at[0] + side - k) % side * units + done[k]
        line[pl.ds(pl.multiple_of(begin, 16), block.shape[0])] = block[...]
        done[k] += block.shape[0]
    both = jnp.concatenate([own[...], other[...]], axis=0)
    sums = jnp.dot(both, line[...], preferred_element_type=jnp.float32).T
    slots = out.shape[1]
    for i in range(out.shape[0]):
        out[i] = sums[i * slots : (i + 1) * slots].astype(jnp.bfloat16)


def down_rows(blocks, x_at, own, other, slots):
    offsets = [k for k in sorted(blocks) for _ in blocks[k]]
    flat = [piece for k in sorted(blocks) for piece in blocks[k]]
    rows = flat[0].shape[1]
    feats, units = own.shape
    whole = pl.BlockSpec(memory_space=pltpu.VMEM)
    return pl.pallas_call(
        functools.partial(down_body, offsets),
        in_specs=[pl.BlockSpec(memory_space=pltpu.SMEM)] + [whole] * (len(flat) + 2),
        out_specs=whole,
        out_shape=jax.ShapeDtypeStruct((rows // slots, slots, 2 * feats), jnp.bfloat16),
        scratch_shapes=[pltpu.VMEM((units, rows), jnp.bfloat16)],
        compiler_params=pltpu.CompilerParams(vmem_limit_bytes=16 * MIB),
        name="down_rows",
    )(x_at, *flat, own, other)


def shift(extent, by):
    return [(i, (i + by) % extent) for i in range(extent)]


def ring_gather(block, extent):
    def send(value, way):
        return lax.ppermute(value, "x", shift(extent, 1 if way == "a" else -1))

    found = {0: [block]}
    ahead = back = block
    for hop in range(1, extent // 2):
        ahead, back = send(ahead, "a"), send(back, "b")
        found[hop], found[extent - hop] = [ahead], [back]
    half = block.shape[0] // 2
    hop = extent // 2
    found[hop] = [send(ahead[:half], "a"), send(back[half:], "b")]
    return found


def build(side):
    def on_device(batch_counts, attn_out, residual_in, norm_gain, w_gate_up, w_down, next_gain):
        slots, width = attn_out.shape
        units = w_gate_up.shape[1]
        feats = w_down.shape[1]
        x_at = lax.axis_index("x")
        core = lax.axis_index("core")
        swap = [(0, 1), (1, 0)]

        partner_gate_up = lax.ppermute(w_gate_up, "core", swap)

        occupied = lax.broadcasted_iota(jnp.int32, (slots, 1), 0) < batch_counts[0]
        summed = residual_in.astype(jnp.float32) + attn_out.astype(jnp.float32)

        sent = norm_rows(attn_out, residual_in, norm_gain, side)
        at = (x_at.reshape(1).astype(jnp.int32), core.reshape(1).astype(jnp.int32))
        sent, at = lax.optimization_barrier((sent, at))
        column = lax.all_to_all(sent, "y", split_axis=0, concat_axis=0, tiled=True)
        partner_gate_up = hold(partner_gate_up)
        by_line = split_lines(w_down.T, side)
        column = column.reshape(side * slots, width)

        line_down = lax.all_to_all(by_line, "y", split_axis=0, concat_axis=0, tiled=True)
        line_down = line_down.reshape(side * feats, side * CORES * units)
        partner_down = lax.ppermute(line_down, "core", swap)

        rows = side * slots
        columns = ring_gather(column, side)
        parts = []
        for batch in BATCHES:
            parts += gate_up([piece for k in batch for piece in columns[k]], w_gate_up, partner_gate_up)
        acts = place_acts(parts, *at).reshape(CORES * units, side * rows)

        blocks = ring_gather(acts, side)
        outgoing = down_rows(blocks, at[0], line_down, partner_down, slots)
        kept = occupied.astype(jnp.float32)
        before = (summed * kept, next_gain * kept, kept)
        outgoing, (held_sum, held_gain, kept) = lax.optimization_barrier((outgoing, before))
        arrived = lax.all_to_all(outgoing, ("x", "y"), split_axis=0, concat_axis=0, tiled=True)
        arrived = arrived.reshape(side, side, slots, CORES * side * feats)
        mine = jnp.sum(arrived.astype(jnp.float32), axis=1).astype(jnp.bfloat16)
        mine = mine.reshape(side, slots, CORES, side, feats)
        mine = jnp.where(core == 0, mine, mine[:, :, ::-1])
        mlp_out = mine.transpose(1, 3, 0, 2, 4).reshape(slots, width)

        updated = held_sum + mlp_out.astype(jnp.float32) * kept
        hidden_out = updated.astype(jnp.bfloat16)
        normed_out = normalize(updated, held_gain).astype(jnp.bfloat16)
        return (hidden_out, normed_out)

    return on_device


def solution(mesh):
    side = math.isqrt(mesh.shape["dp"] // CORES)
    fine = Mesh(mesh.devices.reshape(mesh.shape["groups"], side, side, CORES), ("groups", "y", "x", "core"))
    dp = ("y", "x", "core")
    rows = ("groups",) + dp
    body = build(side)

    return jax.shard_map(
        body,
        mesh=fine,
        in_specs=(P(rows), P(rows, None), P(rows, None), P(), P(None, dp, None), P(None, dp), P()),
        out_specs=(P(rows, None), P(rows, None)),
        check_vma=False,
    )
```
